32 devices in a mesh: expert: 8 (over z, x), mp: 4 (over y, core).
Axes of the slice: x: 2, y: 2, z: 4, core: 2. Of those that a mesh axis runs over, the one named last changes fastest.
Arguments:
- tokens: bfloat16 [2048, 1024], P('expert'), may hold values from -6 to 6
- cotangent: bfloat16 [2048, 1024], P('expert'), may hold values from -6 to 6
- routes: int32 [2048, 2], P('expert'), may hold values from 0 to 7, all different within a row; in each aligned block of 256 rows (0 to 255, 256 to 511, ...) at most 96 rows name the same one
- router_weight: bfloat16 [1024, 8], replicated, may hold values from -0.1875 to 0.1875
- gate_weight: bfloat16 [8, 1024, 3584], P('expert', None, 'mp'), may hold values from -0.1875 to 0.1875
- up_weight: bfloat16 [8, 1024, 3584], P('expert', None, 'mp'), may hold values from -0.6875 to 0.6875
- down_weight: bfloat16 [8, 3584, 1024], P('expert', 'mp'), may hold values from -0.3674842 to 0.3674842
- mlp_in: float32 [3, 16], replicated, may hold values from -3.5 to 3.5
- mlp_bias: float32 [16], replicated, may hold values from -2 to 2
- mlp_out: float32 [16], replicated, may hold values from -1.5 to 1.5
Outputs:
- mixed: bfloat16 [2048, 1024], P('expert', 'mp')
- gate_update: bfloat16 [8, 1024, 3584], P('expert', None, 'mp')
- up_update: bfloat16 [8, 1024, 3584], P('expert', None, 'mp')
- down_update: bfloat16 [8, 3584, 1024], P('expert', 'mp')
- router_update: bfloat16 [1024, 8], replicated
The draws below stay inside these ranges and needn't reach their ends.
Inputs may be any that keep to these rules, and one draw needn't show every extreme that they name: `routes`: in the rows of one index of the expert axis each expert is named at most 96 times; the two experts of a row differ.
All inputs are finite; a program needn't handle non-finite values.
Results may differ from the reference program's by a relative error of at most 0.0057.
Values may be sent and summed in bfloat16 or wider, within the bound.
A program may use at most 128 MiB of HBM per device.

```python
import math
import jax
import jax.numpy as jnp
import numpy as np
from jax import lax

D = 1024
FF = 3584
TOK_DEV = 256
LOPT_UNITS = 16
FEATURES = 3
EXPERTS = 8
CAP = 96
TOKENS = 2048
N_EXPERT = 8


def draw_up_weight(key, part):
    base = jax.random.fold_in(key, 101)
    column_scale = jnp.exp(jax.random.uniform(jax.random.fold_in(base, 1), (FF,), jnp.float32, -1.15, 1.15))
    ramp = jnp.arange(EXPERTS, dtype=jnp.float32) / max(EXPERTS - 1, 1)
    entries = jnp.clip(jax.random.normal(jax.random.fold_in(base, 2), (EXPERTS, D, FF), jnp.float32), -4.0, 4.0)
    expert_scale = 3.0 ** ramp / 1.732
    values = entries * expert_scale[:, None, None] * column_scale[None, None, :] / D ** 0.5
    return values.astype(jnp.bfloat16)


def draw_down_weight(key, part):
    base = jax.random.fold_in(key, 202)
    column_scale = jnp.exp(jax.random.uniform(jax.random.fold_in(base, 1), (D,), jnp.float32, -1.15, 1.15))
    ramp = jnp.arange(EXPERTS, dtype=jnp.float32) / max(EXPERTS - 1, 1)
    entries = jnp.clip(jax.random.normal(jax.random.fold_in(base, 2), (EXPERTS, FF, D), jnp.float32), -4.0, 4.0)
    expert_scale = 3.0 ** ramp / 1.732
    values = entries * expert_scale[:, None, None] * column_scale[None, None, :] / FF ** 0.5
    return values.astype(jnp.bfloat16)


def raised(drawn, key, source, target, shards_of, factor):
    owner, partner = [(jnp.arange(drawn.shape[axis_at]) // (drawn.shape[axis_at] // shards_of)).reshape([-1 if axis == axis_at else 1 for axis in range(drawn.ndim)]) for axis_at in (source, target)]
    chosen = jax.random.permutation(key, shards_of)[partner]
    strong = (owner == chosen) | (owner == (partner + shards_of // 2) % shards_of)
    return jnp.where(strong, factor * drawn, drawn)


def levels(key, extent, pieces, least, largest):
    def one(axis_at, parts):
        heights = jax.random.uniform(jax.random.fold_in(jax.random.fold_in(key, 6), axis_at), (parts,), jnp.float32, least / len(pieces), largest / len(pieces))
        return jnp.repeat(jnp.exp(heights), extent[axis_at] // parts).reshape((-1,) + (1,) * (len(extent) - axis_at - 1))

    level = one(*pieces[0])
    for cut in pieces[1:]:
        level = level * one(*cut)
    return level


def routed_block(rng, own, number, rows, count, top, bound, lean):
    order = jax.random.permutation(rng, count)
    packed, common = shares(count, rows * top, bound, lean, True), shares(count, rows * top, bound, lean, False)
    places = jnp.arange(count)

    def named(tallies, turn):
        used = int((tallies > 0).sum())
        fixed = max(1, used // 4)
        shifted = fixed + (places - fixed + turn * (used - fixed)) % max(1, count - fixed)
        return jnp.zeros((count,), jnp.int32).at[order[jnp.where(places < fixed, places, shifted)]].set(jnp.asarray(tallies, jnp.int32))

    tallies = jnp.where(number % 4 == 0, named(packed, number // 4), named(common, number - number // 4 - 1))
    mixed = jax.random.permutation(jax.random.fold_in(own, 3), count)
    giver, sink = mixed[0:count // 2 * 2:2], mixed[1:count // 2 * 2:2]
    slack = jnp.minimum(tallies[giver] - 1, bound - tallies[sink]) // 2
    slack = jnp.where((giver == order[0]) | (sink == order[0]) | (tallies[sink] == 0), 0, jnp.maximum(slack, 0))
    shifted = jax.random.randint(jax.random.fold_in(own, 4), (count // 2,), 0, 1 << 20) % (slack + 1)
    tallies = tallies.at[giver].add(-shifted).at[sink].add(shifted)
    labels = jnp.searchsorted(jnp.cumsum(tallies), jnp.arange(rows * top), side="right").astype(jnp.int32)
    grid = labels.reshape(top, rows).T
    grid = grid[jax.random.permutation(jax.random.fold_in(own, 1), rows)]
    turn = jax.random.randint(jax.random.fold_in(own, 2), (rows, 1), 0, top)
    return jnp.take_along_axis(grid, (jnp.arange(top)[None, :] + turn) % top, axis=1)


def shares(count, total, most, slope, full):
    weights = [(1 << 20) // math.isqrt(grade ** slope) + 1 for grade in range(1, count + 1)]
    largest = most if full else min(most, max(-(-total // count), total * weights[0] // sum(weights)))
    least = 1 if total - largest >= count - 1 else 0
    given, rest = [largest] + [least] * (count - 1), total - largest - least * (count - 1)
    while rest > 0:
        movable = [i for i in range(1, count) if given[i] < largest] or [i for i in range(1, count) if given[i] < most]
        whole, budget = sum([weights[i] for i in movable]), rest
        for i in movable:
            more = min(most - given[i], max(1, budget * weights[i] // whole), rest)
            given[i] = given[i] + more
            rest = rest - more
    return np.array(given)


def centred(own_key, shape, deviation, most, cuts=(), kind=jnp.bfloat16):
    gain = levels(own_key, shape, cuts, -0.22, 0.18) if cuts else 1.0
    values = jax.random.normal(own_key, shape, jnp.float32) * deviation * gain
    return jnp.minimum(jnp.maximum(values, -most), most).astype(kind)


def heavy_noise(key, extent, spread, reach, cuts, heavy, kind=jnp.bfloat16):
    result = spread * jax.random.normal(key, extent, jnp.float32)
    if cuts:
        result = result * levels(key, extent, cuts, -0.22, 0.18)
    return jnp.clip(raised(result, jax.random.fold_in(key, 3), *heavy), -reach, reach).astype(kind)


def setup_inputs(seed: int = 0) -> dict:
    splits = jax.random.split(jax.random.key(seed), 11)
    tokens = centred(splits[0], (TOKENS, D), 1.0, 6.0, ((0, 8),))
    cotangent = heavy_noise(splits[1], (TOKENS, D), 1.0, 6.0, ((0, 8),), (0, 1, 8, 2.0))
    routes_keys = jax.random.split(jax.random.fold_in(splits[2], 1), TOKENS // TOK_DEV)
    routes_turns = jax.random.permutation(jax.random.fold_in(splits[2], 3), TOKENS // TOK_DEV)
    routes = jax.vmap(lambda own, number: routed_block(jax.random.fold_in(splits[2], 2), own, number, TOK_DEV, EXPERTS, 2, CAP, 2))(routes_keys, routes_turns).reshape((TOKENS, 2))
    router_weight = centred(splits[3], (D, EXPERTS), D ** -0.5, 0.1875)
    gate_weight = centred(splits[4], (EXPERTS, D, FF), D ** -0.5, 0.1875, ((0, 8), (2, 4)))
    up_weight = draw_up_weight(jax.random.fold_in(splits[10], 71), 0)
    down_weight = draw_down_weight(jax.random.fold_in(splits[10], 71), 0)
    mlp_in = centred(splits[7], (FEATURES, LOPT_UNITS), FEATURES ** -0.5, 3.5, (), jnp.float32)
    mlp_bias = centred(splits[8], (LOPT_UNITS,), 0.5, 2.0, (), jnp.float32)
    mlp_out = centred(splits[9], (LOPT_UNITS,), LOPT_UNITS ** -0.5, 1.5, (), jnp.float32)
    return {"tokens": tokens, "cotangent": cotangent, "routes": routes, "router_weight": router_weight, "gate_weight": gate_weight, "up_weight": up_weight, "down_weight": down_weight, "mlp_in": mlp_in, "mlp_bias": mlp_bias, "mlp_out": mlp_out}


EPSILON = 1e-06

def learned_step(gradient, weight, weight_scale, grad_rms, mlp_in, mlp_bias, mlp_out):
    feat_grad = gradient / grad_rms
    feat_weight = weight.astype(jnp.float32) * weight_scale
    feat_tanh = jnp.tanh(feat_grad)
    summed = jnp.zeros_like(feat_grad)
    for neuron in range(mlp_bias.shape[0]):
        hidden = jnp.maximum(mlp_in[0, neuron] * feat_grad + mlp_in[1, neuron] * feat_weight + mlp_in[2, neuron] * feat_tanh + mlp_bias[neuron], 0.0)
        summed = summed + mlp_out[neuron] * hidden
    return summed.astype(jnp.bfloat16)

def expert_pass(operands):
    rows_x, rows_dy, w_gate, w_up, w_down = operands
    act_gate = jnp.dot(rows_x, w_gate, preferred_element_type=jnp.float32)
    act_up = jnp.dot(rows_x, w_up, preferred_element_type=jnp.float32)
    sigmoid_gate = jax.nn.sigmoid(act_gate)
    silu_gate = act_gate * sigmoid_gate
    hidden = (silu_gate * act_up).astype(jnp.bfloat16)
    expert_out = jnp.dot(hidden, w_down, preferred_element_type=jnp.float32).astype(jnp.bfloat16)
    grad_down = jnp.dot(hidden.T, rows_dy, preferred_element_type=jnp.float32)
    grad_hidden = jnp.dot(rows_dy, w_down.T, preferred_element_type=jnp.float32)
    d_gate = (grad_hidden * act_up * sigmoid_gate * (1.0 + act_gate * (1.0 - sigmoid_gate))).astype(jnp.bfloat16)
    d_up = (grad_hidden * silu_gate).astype(jnp.bfloat16)
    grad_gate = jnp.dot(rows_x.T, d_gate, preferred_element_type=jnp.float32)
    grad_up = jnp.dot(rows_x.T, d_up, preferred_element_type=jnp.float32)
    return (expert_out, grad_gate, grad_up, grad_down)

def reference(tokens, cotangent, routes, router_weight, gate_weight, up_weight, down_weight, mlp_in, mlp_bias, mlp_out):
    expert_ids = jnp.arange(EXPERTS, dtype=jnp.int32)
    picks = (routes[:, :, None] == expert_ids[None, None, :]).astype(jnp.int32)
    blocks = picks.reshape(N_EXPERT, TOK_DEV * 2, EXPERTS)
    before = jnp.cumsum(blocks, axis=1) - blocks
    places = lax.optimization_barrier(jnp.sum(before * blocks, axis=2)).reshape(TOKENS, 2).astype(jnp.int32)
    sources = (jnp.arange(TOKENS, dtype=jnp.int32) // TOK_DEV)[:, None]
    slot_rows = (sources * CAP + places).astype(jnp.int32)
    chosen = picks.astype(jnp.float32)
    logits = jnp.dot(tokens, router_weight, preferred_element_type=jnp.float32)
    picked = lax.optimization_barrier(jnp.sum(logits[:, None, :] * chosen, axis=2))
    sigmas = jax.nn.sigmoid(picked)
    denominator = lax.optimization_barrier(jnp.sum(sigmas, axis=1, keepdims=True))
    gates = sigmas / denominator
    scaled_cot = (gates[:, :, None] * cotangent.astype(jnp.float32)[:, None, :]).astype(jnp.bfloat16)
    flat_experts = routes.reshape(-1).astype(jnp.int32)
    flat_rows = slot_rows.reshape(-1)
    x_in = jnp.zeros((EXPERTS, EXPERTS * CAP, D), jnp.bfloat16).at[flat_experts, flat_rows].set(jnp.repeat(tokens, 2, axis=0))
    dy_in = jnp.zeros((EXPERTS, EXPERTS * CAP, D), jnp.bfloat16).at[flat_experts, flat_rows].set(scaled_cot.reshape(TOKENS * 2, D))
    expert_out, grad_gate, grad_up, grad_down = lax.map(expert_pass, (x_in, dy_in, gate_weight, up_weight, down_weight))
    routed = expert_out[flat_experts, flat_rows].astype(jnp.float32).reshape(TOKENS, 2, D)
    mixed = (tokens.astype(jnp.float32) + gates[:, 0:1] * routed[:, 0] + gates[:, 1:2] * routed[:, 1]).astype(jnp.bfloat16)
    gate_grads = lax.optimization_barrier(jnp.sum(cotangent.astype(jnp.float32)[:, None, :] * routed, axis=2))
    mean_part = lax.optimization_barrier(jnp.sum(gates * gate_grads, axis=1, keepdims=True))
    sigma_grads = (gate_grads - mean_part) / denominator
    logit_grads = sigma_grads * sigmas * (1.0 - sigmas)
    dense_grads = lax.optimization_barrier(jnp.sum(logit_grads[:, :, None] * chosen, axis=1)).astype(jnp.bfloat16)
    router_grad = jnp.dot(tokens.T, dense_grads, preferred_element_type=jnp.float32)
    total_count = EXPERTS * D * FF
    gate_rms = jnp.sqrt(jnp.sum(grad_gate * grad_gate) / total_count + EPSILON)
    up_rms = jnp.sqrt(jnp.sum(grad_up * grad_up) / total_count + EPSILON)
    down_rms = jnp.sqrt(jnp.sum(grad_down * grad_down) / total_count + EPSILON)
    router_rms = jnp.sqrt(jnp.sum(router_grad * router_grad) / (D * EXPERTS) + EPSILON)

    def expert_updates(operands):
        g_gate, g_up, g_down, w_gate, w_up, w_down = operands
        return (learned_step(g_gate, w_gate, D ** 0.5, gate_rms, mlp_in, mlp_bias, mlp_out), learned_step(g_up, w_up, D ** 0.5, up_rms, mlp_in, mlp_bias, mlp_out), learned_step(g_down, w_down, FF ** 0.5, down_rms, mlp_in, mlp_bias, mlp_out))
    gate_update, up_update, down_update = lax.map(expert_updates, (grad_gate, grad_up, grad_down, gate_weight, up_weight, down_weight))
    router_update = learned_step(router_grad, router_weight, D ** 0.5, router_rms, mlp_in, mlp_bias, mlp_out)
    return (mixed, gate_update, up_update, down_update, router_update)
```

```python
import functools

import jax
import jax.numpy as jnp
from jax import lax
from jax.experimental import pallas as pl
from jax.experimental.pallas import tpu as pltpu
from jax.sharding import PartitionSpec as P

EPSILON = 1e-06
LANES = 128
CHUNK = 128
MESH = pl.DeviceIdType.MESH
F32 = jnp.float32
BF16 = jnp.bfloat16


def lane(i, size=LANES):
    return pl.ds(pl.multiple_of(i * size, LANES), size)


def dot(a, b):
    return jnp.dot(a, b, preferred_element_type=F32)


def dot_nt(a, b):
    return lax.dot_general(a, b, (((1,), (1,)), ((), ())), preferred_element_type=F32)


def dot_tn(a, b):
    return lax.dot_general(a, b, (((0,), (0,)), ((), ())), preferred_element_type=F32)


def squares(x):
    return jnp.sum((x * x).reshape(-1, 8, LANES), axis=0)


def every(lo, hi, body):
    def step(i, _):
        body(i)
        return 0

    lax.fori_loop(lo, hi, step, 0)


def fill_table(units, table, mlp_in, mlp_bias, mlp_out):
    total = jnp.zeros((8, LANES), F32)
    for j in range(units):
        bias = jnp.full((8, LANES), mlp_bias[j], F32)
        out = jnp.full((8, LANES), mlp_out[j], F32)
        for k in range(3):
            table[k * units + j] = jnp.full((8, LANES), mlp_in[k, j], F32)
        table[3 * units + j] = -bias
        table[4 * units + j] = out
        total = total + out * bias
    table[5 * units] = total


def network(units, table, f0, f1):
    rows = f0.shape[0]

    def coef(i):
        return jnp.concatenate([table[i]] * (rows // 8), axis=0)

    f2 = jnp.tanh(f0)
    acc = coef(5 * units)
    for j in range(units):
        y = coef(j) * f0 + coef(units + j) * f1 + coef(2 * units + j) * f2
        acc = acc + coef(4 * units + j) * jnp.maximum(y, coef(3 * units + j))
    return acc.astype(BF16)


def inverse_rms(tile, count):
    total = jnp.sum(jnp.sum(tile, axis=0, keepdims=True), axis=1, keepdims=True)
    return jnp.broadcast_to(1.0 / jnp.sqrt(total / count + EPSILON), (8, LANES))


def tall(tile, rows):
    return jnp.concatenate([tile] * (rows // 8), axis=0)


def to_row(column):
    size = column.shape[0]
    r = lax.broadcasted_iota(jnp.int32, (size, LANES), 0)
    c = lax.broadcasted_iota(jnp.int32, (size, LANES), 1)
    return jnp.sum(jnp.where(r == c, column, 0.0), axis=0, keepdims=True)


def to_column(row, size):
    r = lax.broadcasted_iota(jnp.int32, (size, row.shape[1]), 0)
    c = lax.broadcasted_iota(jnp.int32, (size, row.shape[1]), 1)
    return jnp.sum(jnp.where(r == c, row, 0.0), axis=1, keepdims=True)


def flip(a, i, n):
    out, bit = 0, 1
    while bit < n:
        out = out + bit * lax.rem(a // bit + i // bit, 2)
        bit *= 2
    return out


def step_kernel(
    n, groups, cap, units, total_count,
    tokens, cot, routes, router, gate_hbm, up_hbm, down_hbm, mlp_in, mlp_bias, mlp_out,
    mixed_ref, down_out, router_out, inv_out, gate_grad, up_grad,
    m0, m1, gates, sx, sdy, rx, rdy, vg, vu, vd, hid, hid_t, rx_t, silu, slope, dcat, inner,
    gd, gg, gu, part, prec, psum, hrec, back, ret, parcel, pmp, psend, pex, norms, nmp, nsend, nex,
    rpart, rex, rsum, rmp, dout, table, inv_down, squared,
    wsem, own, osem, xsem, xhigh, ysem, yhigh, lowsem, highsem, retsem, psem, pesem, nsem, nesem, rsem, rmsem,
):
    me = lax.axis_index("expert")
    col = lax.axis_index("mp")
    parity = lax.rem(col, 2)
    pair = col // 2
    partner = col + 1 - 2 * parity
    highs = groups // 2
    toks, width = tokens.shape
    colw = width // groups
    slots = n * cap
    hidden = vg.shape[1]
    tiles = hidden // LANES
    cols = lane(col, colw)
    power = n & (n - 1) == 0

    def peer_to(i):
        return flip(me, i, n) if power else lax.rem(me + i, n)

    def peer_from(i):
        return flip(me, i, n) if power else lax.rem(me - i + n, n)

    def remote(src, dst, send, recv, expert, mp):
        return pltpu.make_async_remote_copy(
            src_ref=src, dst_ref=dst, send_sem=send, recv_sem=recv,
            device_id=(expert, mp), device_id_type=MESH,
        )

    def rows(e):
        return pl.ds(pl.multiple_of(e * cap, 16), cap)

    barrier = pltpu.get_barrier_semaphore()

    def greet(i):
        pl.semaphore_signal(barrier, inc=1, device_id=(lax.rem(me + i, n), col), device_id_type=MESH)

    def greet_mp(i):
        pl.semaphore_signal(barrier, inc=1, device_id=(me, lax.rem(col + i, groups)), device_id_type=MESH)

    every(1, n, greet)
    every(1, groups, greet_mp)

    loads = [
        pltpu.make_async_copy(gate_hbm, vg, wsem.at[0]),
        pltpu.make_async_copy(up_hbm, vu, wsem.at[1]),
        pltpu.make_async_copy(down_hbm, vd, wsem.at[2]),
    ]
    for load in loads:
        load.start()

    r0, r1 = routes[0:1, :], routes[1:2, :]
    rank = max(n, 16)
    ids = lax.broadcasted_iota(jnp.int32, (rank, toks), 0)
    picks = jnp.where((ids == r0) | (ids == r1), 1.0, 0.0)
    earlier = jnp.where(
        lax.broadcasted_iota(jnp.int32, (toks, toks), 0) < lax.broadcasted_iota(jnp.int32, (toks, toks), 1), 1.0, 0.0
    )
    before = dot(picks.astype(BF16), earlier.astype(BF16)).astype(jnp.int32)
    place = lax.broadcasted_iota(jnp.int32, (cap, toks), 0)
    for e in range(n):
        hit = place == before[e : e + 1, :]
        m0[e * cap : (e + 1) * cap, :] = jnp.where(hit & (r0 == e), 1.0, 0.0).astype(BF16)
        m1[e * cap : (e + 1) * cap, :] = jnp.where(hit & (r1 == e), 1.0, 0.0).astype(BF16)
    both = m0[...] + m1[...]
    sx[...] = dot(both, tokens[:, cols]).astype(BF16)

    def exchange(send, out, sem, high):
        def spread(i):
            peer = peer_to(i)
            return remote(send.at[rows(peer)], out.at[rows(me), cols], sem.at[0, i], sem.at[1, i], peer, col)

        def block(owner, i, send_sem, recv_sem, target):
            ref = out.at[rows(peer_from(i)), lane(owner, colw)]
            return remote(ref, ref, send_sem, recv_sem, me, target)

        def low(i):
            return block(col, i, sem.at[2, i], sem.at[3, i], partner)

        def far(h, i):
            return block(col, i, high.at[0, h - 1, i], high.at[1, h - 1, i], lax.rem(col + 2 * h, groups))

        def forward(h, i):
            owner = lax.rem(col - 2 * h + 2 * groups, groups)
            return block(owner, i, high.at[2, h - 1, i], high.at[3, h - 1, i], partner)

        def share(i):
            for h in range(1, highs):
                far(h, i).start()
            low(i).start()

        def relay(i):
            for h in range(1, highs):
                far(h, i).wait_recv()
                forward(h, i).start()

        def step(i):
            @pl.when((i > 0) & (i < n))
            def _():
                spread(i).wait_recv()

            @pl.when(i < n)
            def _():
                share(i)

            @pl.when(i > 0)
            def _():
                relay(i - 1)

        def arrived(i):
            low(i).wait_recv()
            for h in range(1, highs):
                forward(h, i).wait_recv()

        def sent(i):
            low(i).wait_send()
            for h in range(1, highs):
                far(h, i).wait_send()
                forward(h, i).wait_send()

        return spread, step, arrived, sent

    spread_x, step_x, arrived_x, sent_x = exchange(sx, rx, xsem, xhigh)
    spread_y, step_y, arrived_y, sent_y = exchange(sdy, rdy, ysem, yhigh)

    pl.semaphore_wait(barrier, n - 1 + groups - 1)
    every(1, n, lambda i: spread_x(i).start())
    own_x = pltpu.make_async_copy(sx.at[rows(me)], rx.at[rows(me), cols], own.at[0])
    own_x.start()

    logits = dot_nt(router[...], tokens[...])
    kinds = lax.broadcasted_iota(jnp.int32, (n, toks), 0)
    sigma0 = jax.nn.sigmoid(jnp.sum(jnp.where(kinds == r0, logits, 0.0), axis=0, keepdims=True))
    sigma1 = jax.nn.sigmoid(jnp.sum(jnp.where(kinds == r1, logits, 0.0), axis=0, keepdims=True))
    gates[0:1, :] = sigma0 / (sigma0 + sigma1)
    gates[1:2, :] = sigma1 / (sigma0 + sigma1)
    gates[2:3, :] = 1.0 - sigma0
    gates[3:4, :] = 1.0 - sigma1
    weight = jnp.sum(
        m0[...].astype(F32) * gates[0:1, :] + m1[...].astype(F32) * gates[1:2, :], axis=1, keepdims=True
    )
    sdy[...] = (weight * dot(both, cot[:, cols])).astype(BF16)
    own_x.wait()
    every(1, n, lambda i: spread_y(i).start())
    own_y = pltpu.make_async_copy(sdy.at[rows(me)], rdy.at[rows(me), cols], own.at[1])
    own_y.start()
    fill_table(units, table, mlp_in, mlp_bias, mlp_out)

    every(0, n + 1, step_x)
    every(0, n, arrived_x)
    own_y.wait()
    for load in loads:
        load.wait()

    def forward_tile(j):
        every(j * (n + 1) // tiles, (j + 1) * (n + 1) // tiles, step_y)
        c = lane(j)
        act = dot(rx[...], jnp.concatenate([vg[:, c], vu[:, c]], axis=1))
        act_gate, act_up = act[:, :LANES], act[:, LANES:]
        s = jax.nn.sigmoid(act_gate)
        silu_gate = act_gate * s
        h = silu_gate * act_up
        silu[:, c] = silu_gate
        slope[:, c] = act_up * s * (1.0 + act_gate * (1.0 - s))
        hid[:, c] = h.astype(BF16)
        hid_t[lane(j), :] = h.T.astype(BF16)

    every(0, tiles, forward_tile)

    def turn(j):
        rx_t[lane(j), :] = rx[:, lane(j)].astype(F32).T.astype(BF16)

    every(0, width // LANES, turn)

    def partial(m):
        part[m] = dot(hid[...], vd[:, lane(m, colw)]).astype(BF16)

    every(0, groups, partial)

    def give(q):
        return remote(part.at[2 * q + 1 - parity], prec.at[q], lowsem.at[0, q], lowsem.at[1, q], me, partner)

    every(0, highs, lambda q: give(q).start())
    every(0, n, arrived_y)

    inner[...] = jnp.zeros_like(inner)

    def back_tile(start, size):
        r = pl.ds(pl.multiple_of(start, LANES), size)
        gh = dot_nt(rdy[...], vd[r, :])
        for q in range(size // LANES):
            c = pl.ds(pl.multiple_of(start + q * LANES, LANES), LANES)
            piece = gh[:, q * LANES : (q + 1) * LANES]
            d = pl.multiple_of(2 * (start + q * LANES), LANES)
            dcat[:, pl.ds(d, LANES)] = (piece * slope[:, c]).astype(BF16)
            dcat[:, pl.ds(pl.multiple_of(d + LANES, LANES), LANES)] = (piece * silu[:, c]).astype(BF16)
            inner[...] += piece * hid[:, c].astype(F32)

    every(0, hidden // (2 * LANES), lambda j: back_tile(j * 2 * LANES, 2 * LANES))
    if hidden % (2 * LANES):
        back_tile(hidden - LANES, LANES)

    squared[...] = jnp.zeros_like(squared)

    def down_tile(m):
        c = lane(m, 2 * LANES)
        g = dot(hid_t[...], rdy[:, c])
        gd[:, c] = g
        squared[0] += squares(g[:, :LANES]) + squares(g[:, LANES:])

    every(0, width // (2 * LANES), down_tile)

    for e in range(n):
        parcel[e : e + 1, :] = to_row(jnp.sum(inner[e * cap : (e + 1) * cap, :], axis=1, keepdims=True))
    parcel[n : n + 8, :] = squared[0]

    def across(src, dst, sem, i):
        return remote(src, dst.at[col], sem.at[0, i], sem.at[1, i], me, lax.rem(col + i, groups))

    def around(src, dst, sem, i):
        return remote(src, dst.at[me], sem.at[0, i], sem.at[1, i], peer_to(i), col)

    every(1, groups, lambda i: across(parcel, pmp, psem, i).start())
    pmp[col] = parcel[...]

    def total_of(ref, count):
        acc = ref[0]
        for i in range(1, count):
            acc = acc + ref[i]
        return acc

    every(0, highs, lambda q: give(q).wait_recv())

    def lend(h):
        q = lax.rem(pair + h, highs)
        return remote(psum.at[q], hrec.at[pair], highsem.at[0, h], highsem.at[1, h], me, 2 * q + parity)

    def lend_all(h):
        q = lax.rem(pair + h, highs)
        psum[q] = (part[2 * q + parity].astype(F32) + prec[q].astype(F32)).astype(BF16)
        lend(h).start()

    every(1, highs, lend_all)

    def grad_tile(j):
        g = dot(rx_t[...], dcat[:, lane(j, 2 * LANES)])
        c = lane(j)
        gg[:, c] = g[:, :LANES]
        gu[:, c] = g[:, LANES:]
        squared[1] += squares(g[:, :LANES])
        squared[2] += squares(g[:, LANES:])

    half = tiles // 2
    every(0, half, grad_tile)
    every(1, groups, lambda i: across(parcel, pmp, psem, i).wait_recv())
    psend[...] = total_of(pmp, groups)
    every(1, n, lambda i: around(psend, pex, pesem, i).start())
    pex[me] = psend[...]
    every(half, tiles, grad_tile)
    puts = [
        pltpu.make_async_copy(gg, gate_grad, osem.at[0]),
        pltpu.make_async_copy(gu, up_grad, osem.at[1]),
    ]
    for put in puts:
        put.start()
    norms[0:8, :] = squared[1]
    norms[8:16, :] = squared[2]
    every(1, groups, lambda i: across(norms, nmp, nsem, i).start())
    nmp[col] = norms[...]
    every(1, n, lambda i: around(psend, pex, pesem, i).wait_recv())
    down_norm = pex[0, n : n + 8, :]
    for e in range(1, n):
        down_norm = down_norm + pex[e, n : n + 8, :]
    inv_down[...] = inverse_rms(down_norm, total_count)

    strips = width // LANES
    bands = hidden // CHUNK
    down_scale = float((hidden * groups) ** 0.5)

    def update_band(lo, hi):
        def body(step):
            r = pl.ds(pl.multiple_of((step // strips) * CHUNK, CHUNK), CHUNK)
            c = lane(lax.rem(step, strips))
            f0 = gd[r, c] * tall(inv_down[...], CHUNK)
            dout[r, c] = network(units, table, f0, vd[r, c].astype(F32) * down_scale)

        every(lo * strips, hi * strips, body)

    marks = [i * bands // 7 for i in range(8)]
    update_band(marks[0], marks[1])

    every(1, groups, lambda i: across(norms, nmp, nsem, i).wait_recv())
    nsend[...] = total_of(nmp, groups)
    every(1, n, lambda i: around(nsend, nex, nesem, i).start())
    nex[me] = nsend[...]

    g0, g1 = gates[0:1, :], gates[1:2, :]
    gated0 = jnp.zeros((1, toks), F32)
    gated1 = jnp.zeros((1, toks), F32)
    for e in range(n):
        column = to_column(pex[e, pl.ds(me, 1), :], cap)
        gated0 = gated0 + jnp.sum(column * m0[e * cap : (e + 1) * cap, :].astype(F32), axis=0, keepdims=True)
        gated1 = gated1 + jnp.sum(column * m1[e * cap : (e + 1) * cap, :].astype(F32), axis=0, keepdims=True)
    both_gated = gated0 + gated1
    logit0 = (gated0 - g0 * both_gated) * gates[2:3, :]
    logit1 = (gated1 - g1 * both_gated) * gates[3:4, :]
    dense = jnp.where(ids == r0, logit0, 0.0) + jnp.where(ids == r1, logit1, 0.0)
    rpart[...] = dot(dense.astype(BF16), tokens[:, cols])[:n]
    every(1, n, lambda i: around(rpart, rex, rsem, i).start())
    rex[me] = rpart[...]

    update_band(marks[1], marks[3])

    every(1, highs, lambda h: lend(h).wait_recv())
    summed = part[col].astype(F32) + prec[pair].astype(F32)
    for h in range(1, highs):
        summed = summed + hrec[lax.rem(pair + h, highs)].astype(F32)
    back[...] = summed.astype(BF16)

    def bring(i):
        peer = peer_to(i)
        return remote(back.at[rows(peer)], ret.at[rows(me)], retsem.at[0, i], retsem.at[1, i], peer, col)

    every(1, n, lambda i: bring(i).start())
    own_r = pltpu.make_async_copy(back.at[rows(me)], ret.at[rows(me)], own.at[2])
    own_r.start()

    update_band(marks[3], marks[4])
    every(1, n, lambda i: around(rpart, rex, rsem, i).wait_recv())
    rsum[...] = total_of(rex, n)
    every(1, groups, lambda i: across(rsum, rmp, rmsem, i).start())
    rmp[col] = rsum[...]

    update_band(marks[4], marks[5])
    every(1, n, lambda i: around(nsend, nex, nesem, i).wait_recv())
    both_norms = total_of(nex, n)
    inv_out[0] = inverse_rms(both_norms[0:8, :], total_count)
    inv_out[1] = inverse_rms(both_norms[8:16, :], total_count)

    update_band(marks[5], marks[6])
    every(1, groups, lambda i: across(rsum, rmp, rmsem, i).wait_recv())
    router_norm = jnp.zeros((8, LANES), F32)
    for m in range(groups):
        for s in range(colw // LANES):
            router_norm = router_norm + squares(rmp[m, :, s * LANES : (s + 1) * LANES])
    router_inv = inverse_rms(router_norm, float(n * width))
    for m in range(groups):
        for s in range(colw // LANES):
            c = slice(m * colw + s * LANES, m * colw + (s + 1) * LANES)
            f0 = rmp[m, :, s * LANES : (s + 1) * LANES] * tall(router_inv, n)
            router_out[:, c] = network(units, table, f0, router[:, c].astype(F32) * float(width**0.5))

    update_band(marks[6], marks[7])
    puts.append(pltpu.make_async_copy(dout, down_out, osem.at[2]))
    puts[-1].start()

    own_r.wait()
    every(1, n, lambda i: bring(i).wait_recv())
    mixed = tokens[:, cols].astype(F32)
    mixed = mixed + to_column(g0, toks) * dot_tn(m0[...], ret[...])
    mixed = mixed + to_column(g1, toks) * dot_tn(m1[...], ret[...])
    mixed_ref[...] = mixed.astype(BF16)

    def finish(i):
        spread_x(i).wait_send()
        spread_y(i).wait_send()
        around(psend, pex, pesem, i).wait_send()
        around(nsend, nex, nesem, i).wait_send()
        around(rpart, rex, rsem, i).wait_send()
        bring(i).wait_send()

    def finish_mp(i):
        across(parcel, pmp, psem, i).wait_send()
        across(norms, nmp, nsem, i).wait_send()
        across(rsum, rmp, rmsem, i).wait_send()

    every(1, n, finish)
    every(1, groups, finish_mp)
    every(0, n, sent_x)
    every(0, n, sent_y)
    every(0, highs, lambda q: give(q).wait_send())
    every(1, highs, lambda h: lend(h).wait_send())
    for put in puts:
        put.wait()


def fused_step(tokens, cot, routes, router, w_gate, w_up, w_down, mlp_in, mlp_bias, mlp_out, n, groups, total_count):
    toks, width = tokens.shape
    hidden = w_gate.shape[1]
    cap = -(-(3 * toks // n) // 16) * 16
    slots = n * cap
    colw = width // groups
    highs = groups // 2
    units = mlp_bias.shape[0]
    dma = pltpu.SemaphoreType.DMA
    vmem = pl.BlockSpec(memory_space=pltpu.VMEM)
    smem = pl.BlockSpec(memory_space=pltpu.SMEM)
    hbm = pl.BlockSpec(memory_space=pl.ANY)

    def v(*shape, dtype=BF16):
        return pltpu.VMEM(shape, dtype)

    def f(*shape):
        return pltpu.VMEM(shape, F32)

    lines = n + 8
    up_highs = max(highs - 1, 1)
    return pl.pallas_call(
        functools.partial(step_kernel, n, groups, cap, units, total_count),
        out_shape=(
            jax.ShapeDtypeStruct((toks, colw), BF16),
            jax.ShapeDtypeStruct((hidden, width), BF16),
            jax.ShapeDtypeStruct((n, width), BF16),
            jax.ShapeDtypeStruct((2, 8, LANES), F32),
            jax.ShapeDtypeStruct((width, hidden), F32),
            jax.ShapeDtypeStruct((width, hidden), F32),
        ),
        in_specs=[vmem] * 4 + [hbm] * 3 + [smem] * 3,
        out_specs=(vmem, hbm, vmem, vmem, hbm, hbm),
        scratch_shapes=[
            v(slots, toks), v(slots, toks), f(8, toks),
            v(slots, colw), v(slots, colw), v(slots, width), v(slots, width),
            v(width, hidden), v(width, hidden), v(hidden, width),
            v(slots, hidden), v(hidden, slots), v(width, slots),
            f(slots, hidden), f(slots, hidden), v(slots, 2 * hidden), f(slots, LANES),
            f(hidden, width), f(width, hidden), f(width, hidden),
            v(groups, slots, colw), v(highs, slots, colw), v(highs, slots, colw), v(highs, slots, colw),
            v(slots, colw), v(slots, colw),
            f(lines, LANES), f(groups, lines, LANES), f(lines, LANES), f(n, lines, LANES),
            f(16, LANES), f(groups, 16, LANES), f(16, LANES), f(n, 16, LANES),
            f(n, colw), f(n, n, colw), f(n, colw), f(groups, n, colw),
            v(hidden, width), f(5 * units + 1, 8, LANES), f(8, LANES), f(3, 8, LANES),
            dma((3,)), dma((3,)), dma((3,)),
            dma((4, n)), dma((4, up_highs, n)), dma((4, n)), dma((4, up_highs, n)),
            dma((2, highs)), dma((2, highs)), dma((2, n)),
            dma((2, groups)), dma((2, n)), dma((2, groups)), dma((2, n)), dma((2, n)), dma((2, groups)),
        ],
        compiler_params=pltpu.CompilerParams(
            collective_id=0, has_side_effects=True, vmem_limit_bytes=60 * 1024 * 1024
        ),
        name="fused_step",
    )(tokens, cot, routes, router, w_gate, w_up, w_down, mlp_in, mlp_bias, mlp_out)


def update_kernel(units, scale, inv_ref, mlp_in, mlp_bias, mlp_out, g_ref, w_ref, out_ref, table):
    rows, width = g_ref.shape
    strips = width // LANES

    @pl.when(pl.program_id(0) == 0)
    def _():
        fill_table(units, table, mlp_in, mlp_bias, mlp_out)

    def body(step):
        r = pl.ds(pl.multiple_of((step // strips) * CHUNK, CHUNK), CHUNK)
        c = lane(lax.rem(step, strips))
        f0 = g_ref[r, c] * tall(inv_ref[...], CHUNK)
        out_ref[r, c] = network(units, table, f0, w_ref[r, c].astype(F32) * scale)

    every(0, (rows // CHUNK) * strips, body)


def update(g, w, scale, inv, mlp_in, mlp_bias, mlp_out):
    units = mlp_bias.shape[0]
    rows, width = g.shape
    block = CHUNK
    smem = pl.BlockSpec(memory_space=pltpu.SMEM)
    return pl.pallas_call(
        functools.partial(update_kernel, units, scale),
        grid=(rows // block,),
        out_shape=jax.ShapeDtypeStruct((rows, width), BF16),
        in_specs=[
            pl.BlockSpec((8, LANES), lambda i: (0, 0)), smem, smem, smem,
            pl.BlockSpec((block, width), lambda i: (i, 0)),
            pl.BlockSpec((block, width), lambda i: (i, 0)),
        ],
        out_specs=pl.BlockSpec((block, width), lambda i: (i, 0)),
        scratch_shapes=[pltpu.VMEM((5 * units + 1, 8, LANES), F32)],
        cost_estimate=pl.CostEstimate(
            flops=rows * width * 9 * units, bytes_accessed=rows * width * 8, transcendentals=rows * width
        ),
        name="update",
    )(inv, mlp_in, mlp_bias, mlp_out, g, w)


def on_device(
    tokens, cotangent, routes, router_weight, gate_weight, up_weight, down_weight, mlp_in, mlp_bias, mlp_out
):
    n = lax.axis_size("expert")
    groups = lax.axis_size("mp")
    w_gate, w_up, w_down = gate_weight[0], up_weight[0], down_weight[0]
    width, hidden = w_gate.shape
    total_count = float(n * width * hidden * groups)
    mixed, down_update, router_update, inv, gate_grad, up_grad = fused_step(
        tokens, cotangent, routes.T, router_weight.T, w_gate, w_up, w_down,
        mlp_in, mlp_bias, mlp_out, n, groups, total_count,
    )
    net = (mlp_in, mlp_bias, mlp_out)
    gate_update = update(gate_grad, w_gate, float(width**0.5), inv[0], *net)
    up_update = update(up_grad, w_up, float(width**0.5), inv[1], *net)
    return (mixed, gate_update[None], up_update[None], down_update[None], router_update.T)


def solution(mesh):
    placed = (
        P("expert", None),
        P("expert", None),
        P("expert", None),
        P(),
        P("expert", None, "mp"),
        P("expert", None, "mp"),
        P("expert", "mp", None),
        P(),
        P(),
        P(),
    )
    return jax.shard_map(
        on_device,
        mesh=mesh,
        in_specs=placed,
        out_specs=(
            P("expert", "mp"),
            P("expert", None, "mp"),
            P("expert", None, "mp"),
            P("expert", "mp", None),
            P(),
        ),
        check_vma=False,
    )
```

```python
import functools

import jax
import jax.numpy as jnp
from jax import lax
from jax.experimental import pallas as pl
from jax.experimental.pallas import tpu as pltpu
from jax.sharding import PartitionSpec as P

EPSILON = 1e-06
LANES = 128
CHUNK = 128
MESH = pl.DeviceIdType.MESH
F32 = jnp.float32
BF16 = jnp.bfloat16


def lane(i, size=LANES):
    return pl.ds(pl.multiple_of(i * size, LANES), size)


def dot(a, b):
    return jnp.dot(a, b, preferred_element_type=F32)


def dot_nt(a, b):
    return lax.dot_general(a, b, (((1,), (1,)), ((), ())), preferred_element_type=F32)


def dot_tn(a, b):
    return lax.dot_general(a, b, (((0,), (0,)), ((), ())), preferred_element_type=F32)


def squares(x):
    return jnp.sum((x * x).reshape(-1, 8, LANES), axis=0)


def every(lo, hi, body):
    def step(i, _):
        body(i)
        return 0

    lax.fori_loop(lo, hi, step, 0)


def fill_table(units, table, mlp_in, mlp_bias, mlp_out):
    total = jnp.zeros((8, LANES), F32)
    for j in range(units):
        bias = jnp.full((8, LANES), mlp_bias[j], F32)
        out = jnp.full((8, LANES), mlp_out[j], F32)
        for k in range(3):
            table[k * units + j] = jnp.full((8, LANES), mlp_in[k, j], F32)
        table[3 * units + j] = -bias
        table[4 * units + j] = out
        total = total + out * bias
    table[5 * units] = total


def network(units, table, f0, f1):
    rows = f0.shape[0]

    def coef(i):
        return jnp.concatenate([table[i]] * (rows // 8), axis=0)

    f2 = jnp.tanh(f0)
    acc = coef(5 * units)
    for j in range(units):
        y = coef(j) * f0 + coef(units + j) * f1 + coef(2 * units + j) * f2
        acc = acc + coef(4 * units + j) * jnp.maximum(y, coef(3 * units + j))
    return acc.astype(BF16)


def inverse_rms(tile, count):
    total = jnp.sum(jnp.sum(tile, axis=0, keepdims=True), axis=1, keepdims=True)
    return jnp.broadcast_to(1.0 / jnp.sqrt(total / count + EPSILON), (8, LANES))


def tall(tile, rows):
    return jnp.concatenate([tile] * (rows // 8), axis=0)


def to_row(column):
    size = column.shape[0]
    r = lax.broadcasted_iota(jnp.int32, (size, LANES), 0)
    c = lax.broadcasted_iota(jnp.int32, (size, LANES), 1)
    return jnp.sum(jnp.where(r == c, column, 0.0), axis=0, keepdims=True)


def to_column(row, size):
    r = lax.broadcasted_iota(jnp.int32, (size, row.shape[1]), 0)
    c = lax.broadcasted_iota(jnp.int32, (size, row.shape[1]), 1)
    return jnp.sum(jnp.where(r == c, row, 0.0), axis=1, keepdims=True)


def flip(a, i, n):
    out, bit = 0, 1
    while bit < n:
        out = out + bit * lax.rem(a // bit + i // bit, 2)
        bit *= 2
    return out


def step_kernel(
    n, groups, cap, units, total_count,
    tokens_hbm, cot_hbm, routes_hbm, router_hbm, gate_hbm, up_hbm, down_hbm, mlp_in, mlp_bias, mlp_out,
    mixed_ref, down_out, router_out, inv_gate, inv_up, gate_grad, up_grad,
    tokens, cot, routes, router,
    m0, m1, gates, sx, sdy, rx, rdy, vg, vu, vd, hid, hid_t, rx_t, silu, slope, dcat, inner,
    gd, gg, gu, part, prec, psum, hrec, back, ret, parcel, pmp, psend, pex, norms, nmp, nsend, nex,
    rpart, rex, rsum, rmp, dout, table, inv_down, squared,
    isem, wsem, own, osem, xsem, xhigh, ysem, yhigh, lowsem, highsem, retsem, psem, pesem, nsem, nesem, rsem, rmsem,
):
    me = lax.axis_index("expert")
    col = lax.axis_index("mp")
    parity = lax.rem(col, 2)
    pair = col // 2
    partner = col + 1 - 2 * parity
    highs = groups // 2
    toks, width = tokens.shape
    colw = width // groups
    hidden = vg.shape[1]
    tiles = hidden // LANES
    cols = lane(col, colw)
    power = n & (n - 1) == 0

    def peer_to(i):
        return flip(me, i, n) if power else lax.rem(me + i, n)

    def peer_from(i):
        return flip(me, i, n) if power else lax.rem(me - i + n, n)

    def remote(src, dst, send, recv, expert, mp):
        return pltpu.make_async_remote_copy(
            src_ref=src, dst_ref=dst, send_sem=send, recv_sem=recv,
            device_id=(expert, mp), device_id_type=MESH,
        )

    def rows(e):
        return pl.ds(pl.multiple_of(e * cap, 16), cap)

    barrier = pltpu.get_barrier_semaphore()

    def greet(i):
        pl.semaphore_signal(barrier, inc=1, device_id=(lax.rem(me + i, n), col), device_id_type=MESH)

    def greet_mp(i):
        pl.semaphore_signal(barrier, inc=1, device_id=(me, lax.rem(col + i, groups)), device_id_type=MESH)

    every(1, n, greet)
    every(1, groups, greet_mp)

    pairs = ((tokens_hbm, tokens), (cot_hbm, cot), (routes_hbm, routes), (router_hbm, router))
    inputs = [pltpu.make_async_copy(src, dst, isem.at[k]) for k, (src, dst) in enumerate(pairs)]
    for k in (2, 0, 3, 1):
        inputs[k].start()
    loads = [
        pltpu.make_async_copy(gate_hbm, vg, wsem.at[0]),
        pltpu.make_async_copy(up_hbm, vu, wsem.at[1]),
        pltpu.make_async_copy(down_hbm, vd, wsem.at[2]),
    ]
    for load in loads:
        load.start()

    inputs[2].wait()
    r0, r1 = routes[0:1, :], routes[1:2, :]
    rank = max(n, 16)
    ids = lax.broadcasted_iota(jnp.int32, (rank, toks), 0)
    picks = jnp.where((ids == r0) | (ids == r1), 1.0, 0.0)
    earlier = jnp.where(
        lax.broadcasted_iota(jnp.int32, (toks, toks), 0) < lax.broadcasted_iota(jnp.int32, (toks, toks), 1), 1.0, 0.0
    )
    before = dot(picks.astype(BF16), earlier.astype(BF16)).astype(jnp.int32)
    place = lax.broadcasted_iota(jnp.int32, (cap, toks), 0)
    for e in range(n):
        hit = place == before[e : e + 1, :]
        m0[e * cap : (e + 1) * cap, :] = jnp.where(hit & (r0 == e), 1.0, 0.0).astype(BF16)
        m1[e * cap : (e + 1) * cap, :] = jnp.where(hit & (r1 == e), 1.0, 0.0).astype(BF16)
    both = m0[...] + m1[...]
    inputs[0].wait()
    sx[...] = dot(both, tokens[:, cols]).astype(BF16)

    def exchange(send, out, sem, high):
        def spread(i):
            peer = peer_to(i)
            return remote(send.at[rows(peer)], out.at[rows(me), cols], sem.at[0, i], sem.at[1, i], peer, col)

        def block(owner, i, send_sem, recv_sem, target):
            ref = out.at[rows(peer_from(i)), lane(owner, colw)]
            return remote(ref, ref, send_sem, recv_sem, me, target)

        def low(i):
            return block(col, i, sem.at[2, i], sem.at[3, i], partner)

        def far(h, i):
            return block(col, i, high.at[0, h - 1, i], high.at[1, h - 1, i], lax.rem(col + 2 * h, groups))

        def forward(h, i):
            owner = lax.rem(col - 2 * h + 2 * groups, groups)
            return block(owner, i, high.at[2, h - 1, i], high.at[3, h - 1, i], partner)

        def share(i):
            for h in range(1, highs):
                far(h, i).start()
            low(i).start()

        def relay(i):
            for h in range(1, highs):
                far(h, i).wait_recv()
                forward(h, i).start()

        def step(i):
            spread(i).wait_recv()
            share(i)

        def arrived(i):
            low(i).wait_recv()
            for h in range(1, highs):
                forward(h, i).wait_recv()

        def sent(i):
            low(i).wait_send()
            for h in range(1, highs):
                far(h, i).wait_send()
                forward(h, i).wait_send()

        return spread, share, step, relay, arrived, sent

    spread_x, share_x, step_x, relay_x, arrived_x, sent_x = exchange(sx, rx, xsem, xhigh)
    spread_y, share_y, step_y, relay_y, arrived_y, sent_y = exchange(sdy, rdy, ysem, yhigh)

    pl.semaphore_wait(barrier, n - 1 + groups - 1)
    every(1, n, lambda i: spread_x(i).start())
    own_x = pltpu.make_async_copy(sx.at[rows(me)], rx.at[rows(me), cols], own.at[0])
    own_x.start()

    own_x.wait()
    share_x(0)
    inputs[3].wait()
    logits = dot_nt(router[...], tokens[...])
    kinds = lax.broadcasted_iota(jnp.int32, (n, toks), 0)
    sigma0 = jax.nn.sigmoid(jnp.sum(jnp.where(kinds == r0, logits, 0.0), axis=0, keepdims=True))
    sigma1 = jax.nn.sigmoid(jnp.sum(jnp.where(kinds == r1, logits, 0.0), axis=0, keepdims=True))
    gates[0:1, :] = sigma0 / (sigma0 + sigma1)
    gates[1:2, :] = sigma1 / (sigma0 + sigma1)
    gates[2:3, :] = 1.0 - sigma0
    gates[3:4, :] = 1.0 - sigma1
    weight = jnp.sum(
        m0[...].astype(F32) * gates[0:1, :] + m1[...].astype(F32) * gates[1:2, :], axis=1, keepdims=True
    )
    inputs[1].wait()
    sdy[...] = (weight * dot(both, cot[:, cols])).astype(BF16)
    every(1, n, lambda i: spread_y(i).start())
    own_y = pltpu.make_async_copy(sdy.at[rows(me)], rdy.at[rows(me), cols], own.at[1])
    own_y.start()
    fill_table(units, table, mlp_in, mlp_bias, mlp_out)

    every(1, n, step_x)
    every(0, n, relay_x)
    own_y.wait()
    share_y(0)
    early = n // 2
    every(1, early, step_y)
    for load in loads:
        load.wait()
    every(0, n, arrived_x)

    def forward_tile(j):
        every(early + j * (n - early) // tiles, early + (j + 1) * (n - early) // tiles, step_y)
        c = lane(j)
        act = dot(rx[...], jnp.concatenate([vg[:, c], vu[:, c]], axis=1))
        act_gate, act_up = act[:, :LANES], act[:, LANES:]
        s = jax.nn.sigmoid(act_gate)
        silu_gate = act_gate * s
        h = silu_gate * act_up
        silu[:, c] = silu_gate
        slope[:, c] = act_up * s * (1.0 + act_gate * (1.0 - s))
        hid[:, c] = h.astype(BF16)
        hid_t[lane(j), :] = h.T.astype(BF16)

    every(0, tiles, forward_tile)

    def turn(j):
        rx_t[lane(j), :] = rx[:, lane(j)].astype(F32).T.astype(BF16)

    every(0, width // LANES, turn)
    every(0, n, relay_y)

    def partial(m):
        part[m] = dot(hid[...], vd[:, lane(m, colw)]).astype(BF16)

    every(0, groups, partial)

    def give(q):
        return remote(part.at[2 * q + 1 - parity], prec.at[q], lowsem.at[0, q], lowsem.at[1, q], me, partner)

    every(0, highs, lambda q: give(q).start())
    every(0, n, arrived_y)

    inner[...] = jnp.zeros_like(inner)

    def back_tile(start, size):
        r = pl.ds(pl.multiple_of(start, LANES), size)
        gh = dot_nt(rdy[...], vd[r, :])
        for q in range(size // LANES):
            c = pl.ds(pl.multiple_of(start + q * LANES, LANES), LANES)
            piece = gh[:, q * LANES : (q + 1) * LANES]
            d = pl.multiple_of(2 * (start + q * LANES), LANES)
            dcat[:, pl.ds(d, LANES)] = (piece * slope[:, c]).astype(BF16)
            dcat[:, pl.ds(pl.multiple_of(d + LANES, LANES), LANES)] = (piece * silu[:, c]).astype(BF16)
            inner[...] += piece * hid[:, c].astype(F32)

    every(0, hidden // (2 * LANES), lambda j: back_tile(j * 2 * LANES, 2 * LANES))
    if hidden % (2 * LANES):
        back_tile(hidden - LANES, LANES)

    squared[...] = jnp.zeros_like(squared)

    def down_tile(m):
        c = lane(m, 2 * LANES)
        g = dot(hid_t[...], rdy[:, c])
        gd[:, c] = g
        squared[0] += squares(g[:, :LANES]) + squares(g[:, LANES:])

    every(0, width // (2 * LANES), down_tile)

    for e in range(n):
        parcel[e : e + 1, :] = to_row(jnp.sum(inner[e * cap : (e + 1) * cap, :], axis=1, keepdims=True))
    parcel[n : n + 8, :] = squared[0]

    def across(src, dst, sem, i):
        return remote(src, dst.at[col], sem.at[0, i], sem.at[1, i], me, lax.rem(col + i, groups))

    def around(src, dst, sem, i):
        return remote(src, dst.at[me], sem.at[0, i], sem.at[1, i], peer_to(i), col)

    every(1, groups, lambda i: across(parcel, pmp, psem, i).start())
    pmp[col] = parcel[...]

    def total_of(ref, count):
        acc = ref[0]
        for i in range(1, count):
            acc = acc + ref[i]
        return acc

    every(0, highs, lambda q: give(q).wait_recv())

    def lend(h):
        q = lax.rem(pair + h, highs)
        return remote(psum.at[q], hrec.at[pair], highsem.at[0, h], highsem.at[1, h], me, 2 * q + parity)

    def lend_all(h):
        q = lax.rem(pair + h, highs)
        psum[q] = (part[2 * q + parity].astype(F32) + prec[q].astype(F32)).astype(BF16)
        lend(h).start()

    every(1, highs, lend_all)

    def grad_tile(j):
        g = dot(rx_t[...], dcat[:, lane(j, 2 * LANES)])
        c = lane(j)
        gg[:, c] = g[:, :LANES]
        gu[:, c] = g[:, LANES:]
        squared[1] += squares(g[:, :LANES])
        squared[2] += squares(g[:, LANES:])

    half = tiles // 2
    every(0, half, grad_tile)
    every(1, groups, lambda i: across(parcel, pmp, psem, i).wait_recv())
    psend[...] = total_of(pmp, groups)
    every(1, n, lambda i: around(psend, pex, pesem, i).start())
    pex[me] = psend[...]
    every(half, tiles, grad_tile)
    puts = [
        pltpu.make_async_copy(gg, gate_grad, osem.at[0]),
        pltpu.make_async_copy(gu, up_grad, osem.at[1]),
        pltpu.make_async_copy(dout, down_out, osem.at[2]),
    ]
    puts[0].start()
    puts[1].start()
    norms[0:8, :] = squared[1]
    norms[8:16, :] = squared[2]
    every(1, groups, lambda i: across(norms, nmp, nsem, i).start())
    nmp[col] = norms[...]
    every(1, n, lambda i: around(psend, pex, pesem, i).wait_recv())
    down_norm = pex[0, n : n + 8, :]
    for e in range(1, n):
        down_norm = down_norm + pex[e, n : n + 8, :]
    inv_down[...] = inverse_rms(down_norm, total_count)

    strips = width // LANES
    bands = hidden // CHUNK
    down_scale = float((hidden * groups) ** 0.5)

    def update_band(lo, hi):
        def body(step):
            r = pl.ds(pl.multiple_of((step // strips) * CHUNK, CHUNK), CHUNK)
            c = lane(lax.rem(step, strips))
            f0 = gd[r, c] * tall(inv_down[...], CHUNK)
            dout[r, c] = network(units, table, f0, vd[r, c].astype(F32) * down_scale)

        every(lo * strips, hi * strips, body)

    marks = [i * bands // 7 for i in range(8)]
    update_band(marks[0], marks[1])

    every(1, groups, lambda i: across(norms, nmp, nsem, i).wait_recv())
    nsend[...] = total_of(nmp, groups)
    every(1, n, lambda i: around(nsend, nex, nesem, i).start())
    nex[me] = nsend[...]

    g0, g1 = gates[0:1, :], gates[1:2, :]
    gated0 = jnp.zeros((1, toks), F32)
    gated1 = jnp.zeros((1, toks), F32)
    for e in range(n):
        column = to_column(pex[e, pl.ds(me, 1), :], cap)
        gated0 = gated0 + jnp.sum(column * m0[e * cap : (e + 1) * cap, :].astype(F32), axis=0, keepdims=True)
        gated1 = gated1 + jnp.sum(column * m1[e * cap : (e + 1) * cap, :].astype(F32), axis=0, keepdims=True)
    both_gated = gated0 + gated1
    logit0 = (gated0 - g0 * both_gated) * gates[2:3, :]
    logit1 = (gated1 - g1 * both_gated) * gates[3:4, :]
    dense = jnp.where(ids == r0, logit0, 0.0) + jnp.where(ids == r1, logit1, 0.0)
    rpart[...] = dot(dense.astype(BF16), tokens[:, cols])[:n]
    every(1, n, lambda i: around(rpart, rex, rsem, i).start())
    rex[me] = rpart[...]

    update_band(marks[1], marks[2])

    every(1, highs, lambda h: lend(h).wait_recv())
    summed = part[col].astype(F32) + prec[pair].astype(F32)
    for h in range(1, highs):
        summed = summed + hrec[lax.rem(pair + h, highs)].astype(F32)
    back[...] = summed.astype(BF16)

    def bring(i):
        peer = peer_to(i)
        return remote(back.at[rows(peer)], ret.at[rows(me)], retsem.at[0, i], retsem.at[1, i], peer, col)

    every(1, n, lambda i: bring(i).start())
    own_r = pltpu.make_async_copy(back.at[rows(me)], ret.at[rows(me)], own.at[2])
    own_r.start()

    update_band(marks[2], marks[4])
    every(1, n, lambda i: around(rpart, rex, rsem, i).wait_recv())
    rsum[...] = total_of(rex, n)
    every(1, groups, lambda i: across(rsum, rmp, rmsem, i).start())
    rmp[col] = rsum[...]

    update_band(marks[4], marks[5])
    every(1, n, lambda i: around(nsend, nex, nesem, i).wait_recv())
    both_norms = total_of(nex, n)
    inv_gate[...] = inverse_rms(both_norms[0:8, :], total_count)
    inv_up[...] = inverse_rms(both_norms[8:16, :], total_count)

    update_band(marks[5], marks[6])
    every(1, groups, lambda i: across(rsum, rmp, rmsem, i).wait_recv())
    router_norm = jnp.zeros((8, LANES), F32)
    for m in range(groups):
        for s in range(colw // LANES):
            router_norm = router_norm + squares(rmp[m, :, s * LANES : (s + 1) * LANES])
    router_inv = inverse_rms(router_norm, float(n * width))
    for m in range(groups):
        for s in range(colw // LANES):
            c = slice(m * colw + s * LANES, m * colw + (s + 1) * LANES)
            f0 = rmp[m, :, s * LANES : (s + 1) * LANES] * tall(router_inv, n)
            router_out[:, c] = network(units, table, f0, router[:, c].astype(F32) * float(width**0.5))

    update_band(marks[6], marks[7])
    puts[2].start()

    own_r.wait()
    every(1, n, lambda i: bring(i).wait_recv())
    mixed = tokens[:, cols].astype(F32)
    mixed = mixed + to_column(g0, toks) * dot_tn(m0[...], ret[...])
    mixed = mixed + to_column(g1, toks) * dot_tn(m1[...], ret[...])
    mixed_ref[...] = mixed.astype(BF16)

    def finish(i):
        spread_x(i).wait_send()
        spread_y(i).wait_send()
        around(psend, pex, pesem, i).wait_send()
        around(nsend, nex, nesem, i).wait_send()
        around(rpart, rex, rsem, i).wait_send()
        bring(i).wait_send()

    def finish_mp(i):
        across(parcel, pmp, psem, i).wait_send()
        across(norms, nmp, nsem, i).wait_send()
        across(rsum, rmp, rmsem, i).wait_send()

    every(1, n, finish)
    every(1, groups, finish_mp)
    every(0, n, sent_x)
    every(0, n, sent_y)
    every(0, highs, lambda q: give(q).wait_send())
    every(1, highs, lambda h: lend(h).wait_send())
    for put in puts:
        put.wait()


def fused_step(tokens, cot, routes, router, w_gate, w_up, w_down, mlp_in, mlp_bias, mlp_out, n, groups, total_count):
    toks, width = tokens.shape
    hidden = w_gate.shape[1]
    cap = -(-(3 * toks // n) // 16) * 16
    slots = n * cap
    colw = width // groups
    highs = groups // 2
    units = mlp_bias.shape[0]
    dma = pltpu.SemaphoreType.DMA
    vmem = pl.BlockSpec(memory_space=pltpu.VMEM)
    smem = pl.BlockSpec(memory_space=pltpu.SMEM)
    hbm = pl.BlockSpec(memory_space=pl.ANY)

    def v(*shape, dtype=BF16):
        return pltpu.VMEM(shape, dtype)

    def f(*shape):
        return pltpu.VMEM(shape, F32)

    lines = n + 8
    up_highs = max(highs - 1, 1)
    return pl.pallas_call(
        functools.partial(step_kernel, n, groups, cap, units, total_count),
        out_shape=(
            jax.ShapeDtypeStruct((toks, colw), BF16),
            jax.ShapeDtypeStruct((hidden, width), BF16),
            jax.ShapeDtypeStruct((n, width), BF16),
            jax.ShapeDtypeStruct((8, LANES), F32),
            jax.ShapeDtypeStruct((8, LANES), F32),
            jax.ShapeDtypeStruct((width, hidden), F32),
            jax.ShapeDtypeStruct((width, hidden), F32),
        ),
        in_specs=[hbm] * 7 + [smem] * 3,
        out_specs=(vmem, hbm, vmem, vmem, vmem, hbm, hbm),
        scratch_shapes=[
            v(toks, width), v(toks, width), pltpu.VMEM((2, toks), jnp.int32), v(n, width),
            v(slots, toks), v(slots, toks), f(8, toks),
            v(slots, colw), v(slots, colw), v(slots, width), v(slots, width),
            v(width, hidden), v(width, hidden), v(hidden, width),
            v(slots, hidden), v(hidden, slots), v(width, slots),
            f(slots, hidden), f(slots, hidden), v(slots, 2 * hidden), f(slots, LANES),
            f(hidden, width), f(width, hidden), f(width, hidden),
            v(groups, slots, colw), v(highs, slots, colw), v(highs, slots, colw), v(highs, slots, colw),
            v(slots, colw), v(slots, colw),
            f(lines, LANES), f(groups, lines, LANES), f(lines, LANES), f(n, lines, LANES),
            f(16, LANES), f(groups, 16, LANES), f(16, LANES), f(n, 16, LANES),
            f(n, colw), f(n, n, colw), f(n, colw), f(groups, n, colw),
            v(hidden, width), f(5 * units + 1, 8, LANES), f(8, LANES), f(3, 8, LANES),
            dma((4,)), dma((3,)), dma((3,)), dma((3,)),
            dma((4, n)), dma((4, up_highs, n)), dma((4, n)), dma((4, up_highs, n)),
            dma((2, highs)), dma((2, highs)), dma((2, n)),
            dma((2, groups)), dma((2, n)), dma((2, groups)), dma((2, n)), dma((2, n)), dma((2, groups)),
        ],
        compiler_params=pltpu.CompilerParams(
            collective_id=0, has_side_effects=True, vmem_limit_bytes=60 * 1024 * 1024
        ),
        name="fused_step",
    )(tokens, cot, routes, router, w_gate, w_up, w_down, mlp_in, mlp_bias, mlp_out)


def ordered_table(units, table, mlp_in, mlp_bias, mlp_out, inv, scale):
    outs = [mlp_out[j] for j in range(units)]
    above = [(out > 0.0).astype(jnp.int32) for out in outs]
    positive = sum(above)
    seen = jnp.int32(0)
    total = jnp.zeros((8, LANES), F32)
    for j in range(units):
        slot = jnp.where(above[j] > 0, seen, positive + j - seen)
        seen = seen + above[j]
        size = jnp.full((8, LANES), jnp.abs(outs[j]), F32)
        bias = jnp.full((8, LANES), mlp_bias[j], F32)
        table[slot] = size * jnp.full((8, LANES), mlp_in[0, j], F32) * inv
        table[units + slot] = size * jnp.full((8, LANES), mlp_in[1, j] * scale, F32)
        table[2 * units + slot] = size * jnp.full((8, LANES), mlp_in[2, j], F32)
        table[3 * units + slot] = -(size * bias)
        table[4 * units + slot] = jnp.full((8, LANES), jnp.where(outs[j] > 0.0, 1.0, -1.0), F32)
        total = total + jnp.full((8, LANES), outs[j], F32) * bias
    table[5 * units] = total
    table[5 * units + 1] = inv
    return positive


def ordered_network(units, table, sure, g, w):
    rows = g.shape[0]

    def coef(i):
        return tall(table[i], rows)

    f2 = jnp.tanh(g * coef(5 * units + 1))
    acc = coef(5 * units)
    for j in range(units):
        y = coef(j) * g + coef(units + j) * w + coef(2 * units + j) * f2
        part = jnp.maximum(y, coef(3 * units + j))
        if j < sure:
            acc = acc + part
        elif j == sure:
            acc = acc + coef(4 * units + j) * part
        else:
            acc = acc - part
    return acc.astype(BF16)


def update_kernel(
    units, scale, gate_grad, up_grad, gate_hbm, up_hbm, inv_gate, inv_up, mlp_in, mlp_bias, mlp_out,
    gate_out, up_out, gate_g, up_g, gate_w, up_w, gate_new, up_new, table, gsem, wsem, osem,
):
    width, hidden = gate_grad.shape
    strips = hidden // LANES
    bands = width // CHUNK

    def rows(b):
        return pl.ds(pl.multiple_of(b * CHUNK, CHUNK), CHUNK)

    def load(k, b):
        r = rows(b)
        g, g_ref, w, w_ref = ((gate_grad, gate_g, gate_hbm, gate_w), (up_grad, up_g, up_hbm, up_w))[k]
        return (
            pltpu.make_async_copy(g.at[r], g_ref.at[r], gsem.at[k, b]),
            pltpu.make_async_copy(w.at[r], w_ref.at[r], wsem.at[k, b]),
        )

    def begin(k, b):
        for copy in load(k, b):
            copy.start()

    every(0, bands, lambda b: begin(0, b))
    every(0, bands, lambda b: begin(1, b))

    def tensor(k, g_ref, w_ref, inv, new, out):
        positive = ordered_table(units, table, mlp_in, mlp_bias, mlp_out, inv[...], scale)

        def put(b):
            return pltpu.make_async_copy(new.at[rows(b)], out.at[rows(b)], osem.at[k, b])

        for sure in range(0, units + 1, 2):

            @pl.when(positive // 2 == sure // 2)
            def _():
                def band(b):
                    r = rows(b)
                    for copy in load(k, b):
                        copy.wait()

                    def strip(c):
                        new[r, lane(c)] = ordered_network(
                            units, table, sure, g_ref[r, lane(c)], w_ref[r, lane(c)].astype(F32)
                        )

                    every(0, strips, strip)
                    put(b).start()

                every(0, bands, band)

        return put

    puts = [
        tensor(0, gate_g, gate_w, inv_gate, gate_new, gate_out),
        tensor(1, up_g, up_w, inv_up, up_new, up_out),
    ]
    for put in puts:
        every(0, bands, lambda b: put(b).wait())


def update(gate_grad, up_grad, w_gate, w_up, inv_gate, inv_up, mlp_in, mlp_bias, mlp_out):
    units = mlp_bias.shape[0]
    width, hidden = gate_grad.shape
    smem = pl.BlockSpec(memory_space=pltpu.SMEM)
    vmem = pl.BlockSpec(memory_space=pltpu.VMEM)
    hbm = pl.BlockSpec(memory_space=pl.ANY)
    shape = jax.ShapeDtypeStruct((width, hidden), BF16)
    return pl.pallas_call(
        functools.partial(update_kernel, units, float(width**0.5)),
        out_shape=(shape, shape),
        in_specs=[hbm] * 4 + [vmem] * 2 + [smem] * 3,
        out_specs=(hbm, hbm),
        scratch_shapes=[
            pltpu.VMEM((width, hidden), F32),
            pltpu.VMEM((width, hidden), F32),
            pltpu.VMEM((width, hidden), BF16),
            pltpu.VMEM((width, hidden), BF16),
            pltpu.VMEM((width, hidden), BF16),
            pltpu.VMEM((width, hidden), BF16),
            pltpu.VMEM((5 * units + 2, 8, LANES), F32),
            pltpu.SemaphoreType.DMA((2, width // CHUNK)),
            pltpu.SemaphoreType.DMA((2, width // CHUNK)),
            pltpu.SemaphoreType.DMA((2, width // CHUNK)),
        ],
        compiler_params=pltpu.CompilerParams(vmem_limit_bytes=60 * 1024 * 1024),
        cost_estimate=pl.CostEstimate(
            flops=2 * width * hidden * 9 * units, bytes_accessed=4 * width * hidden,
            transcendentals=2 * width * hidden,
        ),
        name="update",
    )(gate_grad, up_grad, w_gate, w_up, inv_gate, inv_up, mlp_in, mlp_bias, mlp_out)


def on_device(
    tokens, cotangent, routes, router_weight, gate_weight, up_weight, down_weight, mlp_in, mlp_bias, mlp_out
):
    n = lax.axis_size("expert")
    groups = lax.axis_size("mp")
    w_gate, w_up, w_down = gate_weight[0], up_weight[0], down_weight[0]
    width, hidden = w_gate.shape
    total_count = float(n * width * hidden * groups)
    mixed, down_update, router_update, inv_gate, inv_up, gate_grad, up_grad = fused_step(
        tokens, cotangent, routes.T, router_weight.T, w_gate, w_up, w_down,
        mlp_in, mlp_bias, mlp_out, n, groups, total_count,
    )
    gate_update, up_update = update(
        gate_grad, up_grad, w_gate, w_up, inv_gate, inv_up, mlp_in, mlp_bias, mlp_out
    )
    return (mixed, gate_update[None], up_update[None], down_update[None], router_update.T)


def solution(mesh):
    placed = (
        P("expert", None),
        P("expert", None),
        P("expert", None),
        P(),
        P("expert", None, "mp"),
        P("expert", None, "mp"),
        P("expert", "mp", None),
        P(),
        P(),
        P(),
    )
    return jax.shard_map(
        on_device,
        mesh=mesh,
        in_specs=placed,
        out_specs=(
            P("expert", "mp"),
            P("expert", None, "mp"),
            P("expert", None, "mp"),
            P("expert", "mp", None),
            P(),
        ),
        check_vma=False,
    )
```

```python
import functools

import jax
import jax.numpy as jnp
from jax import lax
from jax.experimental import pallas as pl
from jax.experimental.pallas import tpu as pltpu
from jax.sharding import PartitionSpec as P

EPSILON = 1e-06
LANES = 128
CHUNK = 128
MESH = pl.DeviceIdType.MESH
F32 = jnp.float32
BF16 = jnp.bfloat16


def lane(i, size=LANES):
    return pl.ds(pl.multiple_of(i * size, LANES), size)


def dot(a, b):
    return jnp.dot(a, b, preferred_element_type=F32)


def dot_nt(a, b):
    return lax.dot_general(a, b, (((1,), (1,)), ((), ())), preferred_element_type=F32)


def dot_tn(a, b):
    return lax.dot_general(a, b, (((0,), (0,)), ((), ())), preferred_element_type=F32)


def squares(x):
    return jnp.sum((x * x).reshape(-1, 8, LANES), axis=0)


def every(lo, hi, body):
    def step(i, _):
        body(i)
        return 0

    lax.fori_loop(lo, hi, step, 0)


def fill_table(units, table, mlp_in, mlp_bias, mlp_out):
    def splat(value):
        return jnp.full((8, LANES), value, F32)

    outs = [splat(mlp_out[j]) for j in range(units)]
    above = [jnp.where(out > 0.0, 1.0, 0.0) for out in outs]
    positive = above[0]
    for j in range(1, units):
        positive = positive + above[j]
    flipped = positive < units / 2
    turn = jnp.where(flipped, -1.0, 1.0)
    first = [jnp.where(flipped, 1.0 - a, a) for a in above]
    leading = jnp.where(flipped, units - positive, positive)
    slots, seen = [], jnp.zeros((8, LANES), F32)
    total = jnp.zeros((8, LANES), F32)
    for j in range(units):
        slots.append(jnp.where(first[j] > 0.0, seen, leading + j - seen))
        seen = seen + first[j]
        total = total + outs[j] * splat(mlp_bias[j])

    def place(r):
        zero = jnp.zeros((8, LANES), F32)
        sums = [zero] * 5
        for j in range(units):
            here = slots[j] == r.astype(F32)
            size = jnp.abs(outs[j])
            values = [size * splat(mlp_in[k, j]) for k in range(3)]
            values += [-(size * splat(mlp_bias[j])), 2.0 * first[j] - 1.0]
            sums = [a + jnp.where(here, v, zero) for a, v in zip(sums, values)]
        for k in range(5):
            table[k * units + r] = sums[k]

    every(0, units, place)
    table[5 * units] = turn * total
    table[5 * units + 1] = jnp.ones((8, LANES), F32)
    table[5 * units + 2] = turn


def fold_table(units, table, folded, inv, scale):
    folded[...] = table[...]
    for j in range(units):
        folded[j] = table[j] * inv
        folded[units + j] = table[units + j] * scale
    folded[5 * units + 1] = inv


def inverse_rms(tile, count):
    total = jnp.sum(jnp.sum(tile, axis=0, keepdims=True), axis=1, keepdims=True)
    return jnp.broadcast_to(1.0 / jnp.sqrt(total / count + EPSILON), (8, LANES))


def tall(tile, rows):
    return jnp.concatenate([tile] * (rows // 8), axis=0)


def network(units, table, sure, signed, g, w):
    rows = g.shape[0]

    def coef(i):
        return tall(table[i], rows)

    f2 = jnp.tanh(g * coef(5 * units + 1))
    acc = coef(5 * units)
    for j in range(units):
        y = coef(j) * g + coef(units + j) * w + coef(2 * units + j) * f2
        part = jnp.maximum(y, coef(3 * units + j))
        if j < sure:
            acc = acc + part
        elif j < sure + signed:
            acc = acc + coef(4 * units + j) * part
        else:
            acc = acc - part
    return acc


def to_row(column):
    size = column.shape[0]
    r = lax.broadcasted_iota(jnp.int32, (size, LANES), 0)
    c = lax.broadcasted_iota(jnp.int32, (size, LANES), 1)
    return jnp.sum(jnp.where(r == c, column, 0.0), axis=0, keepdims=True)


def to_column(row, size):
    r = lax.broadcasted_iota(jnp.int32, (size, row.shape[1]), 0)
    c = lax.broadcasted_iota(jnp.int32, (size, row.shape[1]), 1)
    return jnp.sum(jnp.where(r == c, row, 0.0), axis=1, keepdims=True)


def flip(a, i, n):
    out, bit = 0, 1
    while bit < n:
        out = out + bit * lax.rem(a // bit + i // bit, 2)
        bit *= 2
    return out


def step_kernel(
    n, groups, cap, units, total_count,
    tokens_hbm, cot_hbm, routes_hbm, router_hbm, gate_hbm, up_hbm, down_hbm, mlp_in, mlp_bias, mlp_out,
    mixed_ref, down_out, router_out, inv_gate, inv_up, gate_grad, up_grad,
    tokens, cot, routes, router,
    m0, m1, gates, sx, sdy, rx, rdy, vg, vu, vd, hid, hid_t, rx_t, silu, slope, dcat, inner,
    gd, gg, gu, part, prec, psum, hrec, back, ret, parcel, pmp, psend, pex, norm_down, dmp, dsend, dex,
    rpart, rex, rsum, rmp, dout, table, folded, squared,
    isem, wsem, own, osem, xsem, xhigh, ysem, yhigh, lowsem, highsem, retsem, psem, pesem, nsem, nesem, rsem, rmsem,
):
    me = lax.axis_index("expert")
    col = lax.axis_index("mp")
    parity = lax.rem(col, 2)
    pair = col // 2
    partner = col + 1 - 2 * parity
    highs = groups // 2
    toks, width = tokens.shape
    colw = width // groups
    hidden = vg.shape[1]
    tiles = hidden // LANES
    cols = lane(col, colw)
    power = n & (n - 1) == 0

    def peer_to(i):
        return flip(me, i, n) if power else lax.rem(me + i, n)

    def peer_from(i):
        return flip(me, i, n) if power else lax.rem(me - i + n, n)

    def remote(src, dst, send, recv, expert, mp):
        return pltpu.make_async_remote_copy(
            src_ref=src, dst_ref=dst, send_sem=send, recv_sem=recv,
            device_id=(expert, mp), device_id_type=MESH,
        )

    def rows(e):
        return pl.ds(pl.multiple_of(e * cap, 16), cap)

    barrier = pltpu.get_barrier_semaphore()

    def greet(i):
        pl.semaphore_signal(barrier, inc=1, device_id=(lax.rem(me + i, n), col), device_id_type=MESH)

    def greet_mp(i):
        pl.semaphore_signal(barrier, inc=1, device_id=(me, lax.rem(col + i, groups)), device_id_type=MESH)

    every(1, n, greet)
    every(1, groups, greet_mp)

    pairs = ((tokens_hbm, tokens), (cot_hbm, cot), (routes_hbm, routes), (router_hbm, router))
    inputs = [pltpu.make_async_copy(src, dst, isem.at[k]) for k, (src, dst) in enumerate(pairs)]
    for k in (2, 0, 3, 1):
        inputs[k].start()
    loads = [
        pltpu.make_async_copy(gate_hbm, vg, wsem.at[0]),
        pltpu.make_async_copy(up_hbm, vu, wsem.at[1]),
        pltpu.make_async_copy(down_hbm, vd, wsem.at[2]),
    ]
    for load in loads:
        load.start()

    inputs[2].wait()
    r0, r1 = routes[0:1, :], routes[1:2, :]
    rank = max(n, 16)
    ids = lax.broadcasted_iota(jnp.int32, (rank, toks), 0)
    picks = jnp.where((ids == r0) | (ids == r1), 1.0, 0.0)
    earlier = jnp.where(
        lax.broadcasted_iota(jnp.int32, (toks, toks), 0) < lax.broadcasted_iota(jnp.int32, (toks, toks), 1), 1.0, 0.0
    )
    before = dot(picks.astype(BF16), earlier.astype(BF16)).astype(jnp.int32)
    place = lax.broadcasted_iota(jnp.int32, (cap, toks), 0)
    for e in range(n):
        hit = place == before[e : e + 1, :]
        m0[e * cap : (e + 1) * cap, :] = jnp.where(hit & (r0 == e), 1.0, 0.0).astype(BF16)
        m1[e * cap : (e + 1) * cap, :] = jnp.where(hit & (r1 == e), 1.0, 0.0).astype(BF16)
    both = m0[...] + m1[...]
    inputs[0].wait()
    sx[...] = dot(both, tokens[:, cols]).astype(BF16)

    def exchange(send, out, sem, high):
        def spread(i):
            peer = peer_to(i)
            return remote(send.at[rows(peer)], out.at[rows(me), cols], sem.at[0, i], sem.at[1, i], peer, col)

        def block(owner, i, send_sem, recv_sem, target):
            ref = out.at[rows(peer_from(i)), lane(owner, colw)]
            return remote(ref, ref, send_sem, recv_sem, me, target)

        def low(i):
            return block(col, i, sem.at[2, i], sem.at[3, i], partner)

        def far(h, i):
            return block(col, i, high.at[0, h - 1, i], high.at[1, h - 1, i], lax.rem(col + 2 * h, groups))

        def forward(h, i):
            owner = lax.rem(col - 2 * h + 2 * groups, groups)
            return block(owner, i, high.at[2, h - 1, i], high.at[3, h - 1, i], partner)

        def share(i):
            for h in range(1, highs):
                far(h, i).start()
            low(i).start()

        def relay(i):
            for h in range(1, highs):
                far(h, i).wait_recv()
                forward(h, i).start()

        def step(i):
            spread(i).wait_recv()
            share(i)

        def arrived(i):
            low(i).wait_recv()
            for h in range(1, highs):
                forward(h, i).wait_recv()

        def sent(i):
            low(i).wait_send()
            for h in range(1, highs):
                far(h, i).wait_send()
                forward(h, i).wait_send()

        return spread, share, step, relay, arrived, sent

    spread_x, share_x, step_x, relay_x, arrived_x, sent_x = exchange(sx, rx, xsem, xhigh)
    spread_y, share_y, step_y, relay_y, arrived_y, sent_y = exchange(sdy, rdy, ysem, yhigh)

    pl.semaphore_wait(barrier, n - 1 + groups - 1)
    every(1, n, lambda i: spread_x(i).start())
    own_x = pltpu.make_async_copy(sx.at[rows(me)], rx.at[rows(me), cols], own.at[0])
    own_x.start()

    own_x.wait()
    share_x(0)
    inputs[3].wait()
    logits = dot_nt(router[...], tokens[...])
    kinds = lax.broadcasted_iota(jnp.int32, (n, toks), 0)
    sigma0 = jax.nn.sigmoid(jnp.sum(jnp.where(kinds == r0, logits, 0.0), axis=0, keepdims=True))
    sigma1 = jax.nn.sigmoid(jnp.sum(jnp.where(kinds == r1, logits, 0.0), axis=0, keepdims=True))
    gates[0:1, :] = sigma0 / (sigma0 + sigma1)
    gates[1:2, :] = sigma1 / (sigma0 + sigma1)
    gates[2:3, :] = 1.0 - sigma0
    gates[3:4, :] = 1.0 - sigma1
    weight = jnp.sum(
        m0[...].astype(F32) * gates[0:1, :] + m1[...].astype(F32) * gates[1:2, :], axis=1, keepdims=True
    )
    inputs[1].wait()
    sdy[...] = (weight * dot(both, cot[:, cols])).astype(BF16)
    every(1, n, lambda i: spread_y(i).start())
    own_y = pltpu.make_async_copy(sdy.at[rows(me)], rdy.at[rows(me), cols], own.at[1])
    own_y.start()
    fill_table(units, table, mlp_in, mlp_bias, mlp_out)

    own_y.wait()
    share_y(0)
    early, near = n // 2, n // 4
    pace = -(-(n - early) * 2 // tiles)
    every(1, early, step_x)
    every(1, near, step_y)
    every(early, n, step_x)
    every(0, early, relay_x)
    every(near, early, step_y)
    every(early, n, relay_x)
    for load in loads:
        load.wait()
    every(0, n, arrived_x)

    def forward_tile(j):
        every(jnp.minimum(early + j * pace, n), jnp.minimum(early + (j + 1) * pace, n), step_y)
        c = lane(j)
        act = dot(rx[...], jnp.concatenate([vg[:, c], vu[:, c]], axis=1))
        act_gate, act_up = act[:, :LANES], act[:, LANES:]
        s = jax.nn.sigmoid(act_gate)
        silu_gate = act_gate * s
        h = silu_gate * act_up
        silu[:, c] = silu_gate
        slope[:, c] = act_up * s * (1.0 + act_gate * (1.0 - s))
        hid[:, c] = h.astype(BF16)
        hid_t[lane(j), :] = h.T.astype(BF16)

    every(0, tiles, forward_tile)

    def turn(j):
        rx_t[lane(j), :] = rx[:, lane(j)].astype(F32).T.astype(BF16)

    every(0, early, relay_y)
    every(0, width // LANES, turn)

    def partial(m):
        part[m] = dot(hid[...], vd[:, lane(m, colw)]).astype(BF16)

    every(0, highs, partial)
    every(early, n, relay_y)
    every(highs, groups, partial)

    def give(q):
        return remote(part.at[2 * q + 1 - parity], prec.at[q], lowsem.at[0, q], lowsem.at[1, q], me, partner)

    every(0, highs, lambda q: give(q).start())
    every(0, n, arrived_y)

    def across(src, dst, sem, i):
        return remote(src, dst.at[col], sem.at[0, i], sem.at[1, i], me, lax.rem(col + i, groups))

    def around(src, dst, sem, i):
        return remote(src, dst.at[me], sem.at[0, i], sem.at[1, i], peer_to(i), col)

    def total_of(ref, count):
        acc = ref[0]
        for i in range(1, count):
            acc = acc + ref[i]
        return acc

    squared[...] = jnp.zeros_like(squared)

    def down_tile(m):
        c = lane(m, 2 * LANES)
        g = dot(hid_t[...], rdy[:, c])
        gd[:, c] = g
        squared[0] += squares(g[:, :LANES]) + squares(g[:, LANES:])

    every(0, width // (2 * LANES), down_tile)
    norm_down[...] = squared[0]
    every(1, groups, lambda i: across(norm_down, dmp, psem, i).start())
    dmp[col] = norm_down[...]

    every(0, highs, lambda q: give(q).wait_recv())

    def lend(h, k):
        q = lax.rem(pair + h, highs)
        part_rows = pl.ds(k * (n * cap // 2), n * cap // 2)
        return remote(
            psum.at[q, part_rows], hrec.at[pair, part_rows],
            highsem.at[0, k, h], highsem.at[1, k, h], me, 2 * q + parity,
        )

    def lend_first(h):
        q = lax.rem(pair + h, highs)
        psum[q] = (part[2 * q + parity].astype(F32) + prec[q].astype(F32)).astype(BF16)
        lend(h, 0).start()

    every(1, highs, lend_first)

    inner[...] = jnp.zeros_like(inner)

    def back_tile(start, size):
        r = pl.ds(pl.multiple_of(start, LANES), size)
        gh = dot_nt(rdy[...], vd[r, :])
        for q in range(size // LANES):
            c = pl.ds(pl.multiple_of(start + q * LANES, LANES), LANES)
            piece = gh[:, q * LANES : (q + 1) * LANES]
            d = pl.multiple_of(2 * (start + q * LANES), LANES)
            dcat[:, pl.ds(d, LANES)] = (piece * slope[:, c]).astype(BF16)
            dcat[:, pl.ds(pl.multiple_of(d + LANES, LANES), LANES)] = (piece * silu[:, c]).astype(BF16)
            inner[...] += piece * hid[:, c].astype(F32)

    every(0, hidden // (2 * LANES), lambda j: back_tile(j * 2 * LANES, 2 * LANES))
    if hidden % (2 * LANES):
        back_tile(hidden - LANES, LANES)
    for e in range(n):
        parcel[e : e + 1, :] = to_row(jnp.sum(inner[e * cap : (e + 1) * cap, :], axis=1, keepdims=True))

    every(1, groups, lambda i: across(norm_down, dmp, psem, i).wait_recv())
    dsend[...] = total_of(dmp, groups)
    every(1, n, lambda i: around(dsend, dex, pesem, i).start())
    dex[me] = dsend[...]

    def grad_tile(j):
        g = dot(rx_t[...], dcat[:, lane(j, 2 * LANES)])
        c = lane(j)
        gg[:, c] = g[:, :LANES]
        gu[:, c] = g[:, LANES:]
        squared[1] += squares(g[:, :LANES])
        squared[2] += squares(g[:, LANES:])

    every(0, tiles, grad_tile)
    puts = [
        pltpu.make_async_copy(gg, gate_grad, osem.at[0]),
        pltpu.make_async_copy(gu, up_grad, osem.at[1]),
        pltpu.make_async_copy(dout, down_out, osem.at[2]),
    ]
    puts[0].start()
    puts[1].start()
    parcel[n : n + 8, :] = squared[1]
    parcel[n + 8 : n + 16, :] = squared[2]
    every(1, groups, lambda i: across(parcel, pmp, nsem, i).start())
    every(1, highs, lambda h: lend(h, 1).start())
    pmp[col] = parcel[...]
    every(1, n, lambda i: around(dsend, dex, pesem, i).wait_recv())
    fold_table(
        units, table, folded, inverse_rms(total_of(dex, n), total_count), float((hidden * groups) ** 0.5)
    )

    strips = width // LANES
    bands = hidden // CHUNK

    def balanced(ref, g, w):
        value = network(units, ref, units // 2, units - units // 2, g, w)
        return (value * tall(table[5 * units + 2], g.shape[0])).astype(BF16)

    def update_band(lo, hi):
        def body(step):
            r = pl.ds(pl.multiple_of((step // strips) * CHUNK, CHUNK), CHUNK)
            c = lane(lax.rem(step, strips))
            dout[r, c] = balanced(folded, gd[r, c], vd[r, c].astype(F32))

        every(lo * strips, hi * strips, body)

    marks = [i * bands // 7 for i in range(8)]
    update_band(marks[0], marks[1])

    every(1, groups, lambda i: across(parcel, pmp, nsem, i).wait_recv())
    psend[...] = total_of(pmp, groups)
    every(1, n, lambda i: around(psend, pex, nesem, i).start())
    pex[me] = psend[...]

    update_band(marks[1], marks[3])
    every(1, n, lambda i: around(psend, pex, nesem, i).wait_recv())
    both_norms = pex[0, n : n + 16, :]
    for e in range(1, n):
        both_norms = both_norms + pex[e, n : n + 16, :]
    inv_gate[...] = inverse_rms(both_norms[0:8, :], total_count)
    inv_up[...] = inverse_rms(both_norms[8:16, :], total_count)

    g0, g1 = gates[0:1, :], gates[1:2, :]
    gated0 = jnp.zeros((1, toks), F32)
    gated1 = jnp.zeros((1, toks), F32)
    for e in range(n):
        column = to_column(pex[e, pl.ds(me, 1), :], cap)
        gated0 = gated0 + jnp.sum(column * m0[e * cap : (e + 1) * cap, :].astype(F32), axis=0, keepdims=True)
        gated1 = gated1 + jnp.sum(column * m1[e * cap : (e + 1) * cap, :].astype(F32), axis=0, keepdims=True)
    both_gated = gated0 + gated1
    logit0 = (gated0 - g0 * both_gated) * gates[2:3, :]
    logit1 = (gated1 - g1 * both_gated) * gates[3:4, :]
    dense = jnp.where(ids == r0, logit0, 0.0) + jnp.where(ids == r1, logit1, 0.0)
    rpart[...] = dot(dense.astype(BF16), tokens[:, cols])[:n]
    every(1, n, lambda i: around(rpart, rex, rsem, i).start())
    rex[me] = rpart[...]

    every(1, highs, lambda h: lend(h, 0).wait_recv())
    every(1, highs, lambda h: lend(h, 1).wait_recv())
    summed = part[col].astype(F32) + prec[pair].astype(F32)
    for h in range(1, highs):
        summed = summed + hrec[lax.rem(pair + h, highs)].astype(F32)
    back[...] = summed.astype(BF16)

    def bring(i):
        peer = peer_to(i)
        return remote(back.at[rows(peer)], ret.at[rows(me)], retsem.at[0, i], retsem.at[1, i], peer, col)

    every(1, n, lambda i: bring(i).start())
    own_r = pltpu.make_async_copy(back.at[rows(me)], ret.at[rows(me)], own.at[2])
    own_r.start()

    update_band(marks[3], marks[5])
    every(1, n, lambda i: around(rpart, rex, rsem, i).wait_recv())
    rsum[...] = total_of(rex, n)
    every(1, groups, lambda i: across(rsum, rmp, rmsem, i).start())
    rmp[col] = rsum[...]

    update_band(marks[5], marks[6])
    every(1, groups, lambda i: across(rsum, rmp, rmsem, i).wait_recv())
    router_norm = jnp.zeros((8, LANES), F32)
    for m in range(groups):
        for s in range(colw // LANES):
            router_norm = router_norm + squares(rmp[m, :, s * LANES : (s + 1) * LANES])
    router_inv = inverse_rms(router_norm, float(n * width))
    for m in range(groups):
        for s in range(colw // LANES):
            c = slice(m * colw + s * LANES, m * colw + (s + 1) * LANES)
            f0 = rmp[m, :, s * LANES : (s + 1) * LANES] * tall(router_inv, n)
            router_out[:, c] = balanced(table, f0, router[:, c].astype(F32) * float(width**0.5))

    update_band(marks[6], marks[7])
    puts[2].start()

    own_r.wait()
    every(1, n, lambda i: bring(i).wait_recv())
    mixed = tokens[:, cols].astype(F32)
    mixed = mixed + to_column(g0, toks) * dot_tn(m0[...], ret[...])
    mixed = mixed + to_column(g1, toks) * dot_tn(m1[...], ret[...])
    mixed_ref[...] = mixed.astype(BF16)

    def finish(i):
        spread_x(i).wait_send()
        spread_y(i).wait_send()
        around(dsend, dex, pesem, i).wait_send()
        around(psend, pex, nesem, i).wait_send()
        around(rpart, rex, rsem, i).wait_send()
        bring(i).wait_send()

    def finish_mp(i):
        across(norm_down, dmp, psem, i).wait_send()
        across(parcel, pmp, nsem, i).wait_send()
        across(rsum, rmp, rmsem, i).wait_send()

    every(1, n, finish)
    every(1, groups, finish_mp)
    every(0, n, sent_x)
    every(0, n, sent_y)
    every(0, highs, lambda q: give(q).wait_send())
    every(1, highs, lambda h: lend(h, 0).wait_send())
    every(1, highs, lambda h: lend(h, 1).wait_send())
    for put in puts:
        put.wait()


def fused_step(tokens, cot, routes, router, w_gate, w_up, w_down, mlp_in, mlp_bias, mlp_out, n, groups, total_count):
    toks, width = tokens.shape
    hidden = w_gate.shape[1]
    cap = -(-(3 * toks // n) // 16) * 16
    slots = n * cap
    colw = width // groups
    highs = groups // 2
    units = mlp_bias.shape[0]
    dma = pltpu.SemaphoreType.DMA
    vmem = pl.BlockSpec(memory_space=pltpu.VMEM)
    smem = pl.BlockSpec(memory_space=pltpu.SMEM)
    hbm = pl.BlockSpec(memory_space=pl.ANY)

    def v(*shape, dtype=BF16):
        return pltpu.VMEM(shape, dtype)

    def f(*shape):
        return pltpu.VMEM(shape, F32)

    lines = n + 16
    up_highs = max(highs - 1, 1)
    return pl.pallas_call(
        functools.partial(step_kernel, n, groups, cap, units, total_count),
        out_shape=(
            jax.ShapeDtypeStruct((toks, colw), BF16),
            jax.ShapeDtypeStruct((hidden, width), BF16),
            jax.ShapeDtypeStruct((n, width), BF16),
            jax.ShapeDtypeStruct((8, LANES), F32),
            jax.ShapeDtypeStruct((8, LANES), F32),
            jax.ShapeDtypeStruct((width, hidden), F32),
            jax.ShapeDtypeStruct((width, hidden), F32),
        ),
        in_specs=[hbm] * 7 + [smem] * 3,
        out_specs=(vmem, hbm, vmem, vmem, vmem, hbm, hbm),
        scratch_shapes=[
            v(toks, width), v(toks, width), pltpu.VMEM((2, toks), jnp.int32), v(n, width),
            v(slots, toks), v(slots, toks), f(8, toks),
            v(slots, colw), v(slots, colw), v(slots, width), v(slots, width),
            v(width, hidden), v(width, hidden), v(hidden, width),
            v(slots, hidden), v(hidden, slots), v(width, slots),
            f(slots, hidden), f(slots, hidden), v(slots, 2 * hidden), f(slots, LANES),
            f(hidden, width), f(width, hidden), f(width, hidden),
            v(groups, slots, colw), v(highs, slots, colw), v(highs, slots, colw), v(highs, slots, colw),
            v(slots, colw), v(slots, colw),
            f(lines, LANES), f(groups, lines, LANES), f(lines, LANES), f(n, lines, LANES),
            f(8, LANES), f(groups, 8, LANES), f(8, LANES), f(n, 8, LANES),
            f(n, colw), f(n, n, colw), f(n, colw), f(groups, n, colw),
            v(hidden, width), f(5 * units + 3, 8, LANES), f(5 * units + 3, 8, LANES), f(3, 8, LANES),
            dma((4,)), dma((3,)), dma((3,)), dma((3,)),
            dma((4, n)), dma((4, up_highs, n)), dma((4, n)), dma((4, up_highs, n)),
            dma((2, highs)), dma((2, 2, highs)), dma((2, n)),
            dma((2, groups)), dma((2, n)), dma((2, groups)), dma((2, n)), dma((2, n)), dma((2, groups)),
        ],
        compiler_params=pltpu.CompilerParams(
            collective_id=0, has_side_effects=True, vmem_limit_bytes=60 * 1024 * 1024
        ),
        name="fused_step",
    )(tokens, cot, routes, router, w_gate, w_up, w_down, mlp_in, mlp_bias, mlp_out)


def ordered_table(units, table, mlp_in, mlp_bias, mlp_out, inv, scale):
    outs = [mlp_out[j] for j in range(units)]
    above = [(out > 0.0).astype(jnp.int32) for out in outs]
    positive = sum(above)
    seen = jnp.int32(0)
    total = jnp.zeros((8, LANES), F32)
    for j in range(units):
        slot = jnp.where(above[j] > 0, seen, positive + j - seen)
        seen = seen + above[j]
        size = jnp.full((8, LANES), jnp.abs(outs[j]), F32)
        bias = jnp.full((8, LANES), mlp_bias[j], F32)
        table[slot] = size * jnp.full((8, LANES), mlp_in[0, j], F32) * inv
        table[units + slot] = size * jnp.full((8, LANES), mlp_in[1, j] * scale, F32)
        table[2 * units + slot] = size * jnp.full((8, LANES), mlp_in[2, j], F32)
        table[3 * units + slot] = -(size * bias)
        table[4 * units + slot] = jnp.full((8, LANES), jnp.where(outs[j] > 0.0, 1.0, -1.0), F32)
        total = total + jnp.full((8, LANES), outs[j], F32) * bias
    table[5 * units] = total
    table[5 * units + 1] = inv
    return positive


def update_kernel(
    units, scale, gate_grad, up_grad, gate_hbm, up_hbm, inv_gate, inv_up, mlp_in, mlp_bias, mlp_out,
    mixed_in, down_in, router_in, gate_out, up_out, mixed_out, down_out, router_out, mixed, down, router, gate_g, up_g, gate_w, up_w, gate_new, up_new, table, gsem, wsem, osem, psem,
):
    width, hidden = gate_grad.shape
    strips = hidden // LANES
    bands = width // CHUNK

    def rows(b):
        return pl.ds(pl.multiple_of(b * CHUNK, CHUNK), CHUNK)

    def load(k, b):
        r = rows(b)
        g, g_ref, w, w_ref = ((gate_grad, gate_g, gate_hbm, gate_w), (up_grad, up_g, up_hbm, up_w))[k]
        return (
            pltpu.make_async_copy(g.at[r], g_ref.at[r], gsem.at[k, b]),
            pltpu.make_async_copy(w.at[r], w_ref.at[r], wsem.at[k, b]),
        )

    def begin(k, b):
        for copy in load(k, b):
            copy.start()

    every(0, bands, lambda b: begin(0, b))
    every(0, bands, lambda b: begin(1, b))
    passing = ((mixed_in, mixed, mixed_out), (down_in, down, down_out), (router_in, router, router_out))
    taken = [pltpu.make_async_copy(a, b, psem.at[0, k]) for k, (a, b, _) in enumerate(passing)]
    given = [pltpu.make_async_copy(b, c, psem.at[1, k]) for k, (_, b, c) in enumerate(passing)]
    for copy in taken:
        copy.start()

    def tensor(k, g_ref, w_ref, inv, new, out):
        positive = ordered_table(units, table, mlp_in, mlp_bias, mlp_out, inv[...], scale)

        def put(b):
            return pltpu.make_async_copy(new.at[rows(b)], out.at[rows(b)], osem.at[k, b])

        for sure in range(0, units + 1, 2):

            @pl.when(positive // 2 == sure // 2)
            def _():
                def band(b):
                    r = rows(b)
                    for copy in load(k, b):
                        copy.wait()

                    def strip(c):
                        new[r, lane(c)] = network(
                            units, table, sure, 1, g_ref[r, lane(c)], w_ref[r, lane(c)].astype(F32)
                        ).astype(BF16)

                    every(0, strips, strip)
                    put(b).start()

                every(0, bands, band)

        return put

    puts = [tensor(0, gate_g, gate_w, inv_gate, gate_new, gate_out)]
    for copy in taken:
        copy.wait()
    for copy in given:
        copy.start()
    puts.append(tensor(1, up_g, up_w, inv_up, up_new, up_out))
    for copy in given:
        copy.wait()
    for put in puts:
        every(0, bands, lambda b: put(b).wait())


def update(gate_grad, up_grad, w_gate, w_up, inv_gate, inv_up, mlp_in, mlp_bias, mlp_out, *passing):
    units = mlp_bias.shape[0]
    width, hidden = gate_grad.shape
    smem = pl.BlockSpec(memory_space=pltpu.SMEM)
    vmem = pl.BlockSpec(memory_space=pltpu.VMEM)
    hbm = pl.BlockSpec(memory_space=pl.ANY)
    shape = jax.ShapeDtypeStruct((width, hidden), BF16)
    return pl.pallas_call(
        functools.partial(update_kernel, units, float(width**0.5)),
        out_shape=(shape, shape) + tuple(jax.ShapeDtypeStruct(x.shape, x.dtype) for x in passing),
        in_specs=[hbm] * 4 + [vmem] * 2 + [smem] * 3 + [hbm] * 3,
        out_specs=(hbm,) * 5,
        scratch_shapes=[pltpu.VMEM(x.shape, x.dtype) for x in passing] + [
            pltpu.VMEM((width, hidden), F32),
            pltpu.VMEM((width, hidden), F32),
            pltpu.VMEM((width, hidden), BF16),
            pltpu.VMEM((width, hidden), BF16),
            pltpu.VMEM((width, hidden), BF16),
            pltpu.VMEM((width, hidden), BF16),
            pltpu.VMEM((5 * units + 2, 8, LANES), F32),
            pltpu.SemaphoreType.DMA((2, width // CHUNK)),
            pltpu.SemaphoreType.DMA((2, width // CHUNK)),
            pltpu.SemaphoreType.DMA((2, width // CHUNK)),
            pltpu.SemaphoreType.DMA((2, 3)),
        ],
        compiler_params=pltpu.CompilerParams(vmem_limit_bytes=60 * 1024 * 1024),
        cost_estimate=pl.CostEstimate(
            flops=2 * width * hidden * 9 * units, bytes_accessed=4 * width * hidden,
            transcendentals=2 * width * hidden,
        ),
        name="update",
    )(gate_grad, up_grad, w_gate, w_up, inv_gate, inv_up, mlp_in, mlp_bias, mlp_out, *passing)


def on_device(
    tokens, cotangent, routes, router_weight, gate_weight, up_weight, down_weight, mlp_in, mlp_bias, mlp_out
):
    n = lax.axis_size("expert")
    groups = lax.axis_size("mp")
    w_gate, w_up, w_down = gate_weight[0], up_weight[0], down_weight[0]
    width, hidden = w_gate.shape
    total_count = float(n * width * hidden * groups)
    mixed, down_update, router_update, inv_gate, inv_up, gate_grad, up_grad = fused_step(
        tokens, cotangent, routes.T, router_weight.T, w_gate, w_up, w_down,
        mlp_in, mlp_bias, mlp_out, n, groups, total_count,
    )
    gate_update, up_update, mixed, down_update, router_update = update(
        gate_grad, up_grad, w_gate, w_up, inv_gate, inv_up, mlp_in, mlp_bias, mlp_out,
        mixed, down_update, router_update,
    )
    return (mixed, gate_update[None], up_update[None], down_update[None], router_update.T)


def solution(mesh):
    placed = (
        P("expert", None),
        P("expert", None),
        P("expert", None),
        P(),
        P("expert", None, "mp"),
        P("expert", None, "mp"),
        P("expert", "mp", None),
        P(),
        P(),
        P(),
    )
    return jax.shard_map(
        on_device,
        mesh=mesh,
        in_specs=placed,
        out_specs=(
            P("expert", "mp"),
            P("expert", None, "mp"),
            P("expert", None, "mp"),
            P("expert", "mp", None),
            P(),
        ),
        check_vma=False,
    )
```
